256 devices in a mesh: rep: 2 (over y), gx: 128 (over z, x, core).
Axes of the slice: x: 4, y: 2, z: 16, core: 2. Of those that a mesh axis runs over, the one named last changes fastest.
The devices are a block of a 4x16x16 slice.
Arguments:
- positions: float32 [3, 393216], P(None, ('rep', 'gx')), parts along dimension 1, may hold values from 0 to 768
- velocities: float32 [3, 393216], P(None, ('rep', 'gx')), parts along dimension 1, may hold values from -9 to 9
- atom_params: float32 [4, 393216], P(None, ('rep', 'gx')), parts along dimension 1, may hold values from -1 to 2, as said below
- pair_list: int32 [3, 4325376], P(None, ('rep', 'gx')), parts along dimension 1, may hold values from 0 to 479, as said below
- pair_count: int32 [256], P(('rep', 'gx')), parts along dimension 0, may hold values from 2112 to 16896, as said below
- exclusion: int32 [4, 4325376], P(None, ('rep', 'gx')), parts along dimension 1, may hold values from 0 to 65535, as said below
- halo_far: int32 [24576], P(('rep', 'gx')), parts along dimension 0, may hold values from 0 to 191, as said below
- box_lengths: float32 [6], P('rep'), parts along dimension 0, may hold values from 12 to 768
- extended_variables: float32 [8], P('rep'), parts along dimension 0, may hold values from -0.3 to 0.3
Outputs:
- forces: float32 [3, 393216], P(None, ('rep', 'gx')), parts along dimension 1
- new_velocities: float32 [3, 393216], P(None, ('rep', 'gx')), parts along dimension 1
- new_positions: float32 [3, 393216], P(None, ('rep', 'gx')), parts along dimension 1
- new_coupling: float32 [8], P('rep'), parts along dimension 0
The draws below stay inside these ranges and needn't reach their ends.
There are 2 independent parts, one for each index of `rep`. The reference program is written for one: setup_inputs(seed, part) draws one part's arguments, and reference() takes and returns one part's arrays. A program takes and returns all parts, laid end to end along the dimension named above; each array names one. Nothing has to cross between parts.
Inputs may be any that keep to these rules, and one draw needn't show every extreme that they name: `pair_list`: row 0 is a local cluster 0 to 191, row 1 a slot 0 to 479 of the slot table, row 2 an image code 0 to 8. Over each domain's used columns row 0 never falls (the list is grouped by its first cluster). Unused columns hold valid entries too. `pair_count`: at most 16896; some domain uses all 16896 columns in every draw. `exclusion`: each word holds 16 bits; bit 1 means the atom pair interacts. `halo_far`: 96 distinct local clusters of each domain. `atom_params`: rows 1 to 3 are positive.
All inputs are finite; a program needn't handle non-finite values.
Results may differ from the reference program's by a relative error of at most 0.0003.
Values sent between devices are 32-bit elements; how exact they have to be, the bound alone decides.
A program may use at most 64 MiB of HBM per device.

```python
import math
import jax
import jax.numpy as jnp
import numpy as np
from jax import lax

LX = 2
LY = 12
LZ = 8
CAND = 88
ATOMS_DEV = 1536
PAIRS_DEV = 16896
COPY_PARTICLES = 196608
PAIRS = 2162688
N_GX = 128


def candidate_offsets():
    result = [(0, 0, 0)]
    for shift_y in range(-2, 3):
        for shift_z in range(-2, 3):
            if shift_y > 0 or (shift_y == 0 and shift_z > 0):
                result.append((0, shift_y, shift_z))
    for shift_x in range(1, 4):
        for shift_y in range(-2, 3):
            for shift_z in range(-2, 3):
                result.append((shift_x, shift_y, shift_z))
    return np.array(result, np.int32)


def upper_words():
    result = []
    for word_place in range(4):
        packed_bits = 0
        for bit_place in range(16):
            number = word_place * 16 + bit_place
            if number % 8 > number // 8:
                packed_bits += 1 << bit_place
        result.append(packed_bits)
    return np.array(result, np.int32)


def cluster_sites(key):
    subkeys = jax.random.split(jax.random.fold_in(key, 101), N_GX)
    return jax.vmap(lambda single: jax.random.permutation(single, LX * LY * LZ))(subkeys).astype(jnp.int32)


def box_stretch(key):
    return jax.random.uniform(jax.random.fold_in(key, 202), (3,), jnp.float32, -0.02, 0.02)


def pair_counts(key):
    base_counts = jax.random.randint(jax.random.fold_in(key, 303), (N_GX,), PAIRS_DEV // 8, PAIRS_DEV // 2 + 1)
    dense_counts = jax.random.randint(jax.random.fold_in(key, 304), (N_GX,), 3 * PAIRS_DEV // 4, PAIRS_DEV + 1)
    dense_start = jax.random.randint(jax.random.fold_in(key, 305), (), 0, N_GX)
    distance = (jnp.arange(N_GX, dtype=jnp.int32) - dense_start) % N_GX
    counts = jnp.where(distance < max(N_GX // 8, 1), dense_counts, base_counts)
    return jnp.where(distance == 0, PAIRS_DEV, counts).astype(jnp.int32)


def pair_order(key):
    counts = pair_counts(key)
    subkeys = jax.random.split(jax.random.fold_in(key, 306), N_GX)
    ranks = jax.vmap(lambda single: jax.random.permutation(single, PAIRS_DEV))(subkeys)
    candidate = jnp.arange(PAIRS_DEV, dtype=jnp.int32)[None, :]
    sort_key = jnp.where(ranks < counts[:, None], candidate, candidate + PAIRS_DEV)
    return jnp.argsort(sort_key, axis=1).astype(jnp.int32)


def pair_tables(key):
    site_of = cluster_sites(key)
    cluster_at = jnp.argsort(site_of, axis=1).astype(jnp.int32)
    plane_size = LY * LZ
    clusters = LX * plane_size
    offsets = jnp.asarray(candidate_offsets())
    layer_x = (site_of // plane_size)[:, :, None]
    layer_y = (site_of // LZ % LY)[:, :, None]
    layer_z = (site_of % LZ)[:, :, None]
    target_x = layer_x + offsets[:, 0]
    raw_y = layer_y + offsets[:, 1]
    raw_z = layer_z + offsets[:, 2]
    wrap_y = (raw_y >= LY).astype(jnp.int32) - (raw_y < 0).astype(jnp.int32)
    wrap_z = (raw_z >= LZ).astype(jnp.int32) - (raw_z < 0).astype(jnp.int32)
    target_y = raw_y - wrap_y * LY
    target_z = raw_z - wrap_z * LZ
    image_code = (wrap_y + 1) * 3 + wrap_z + 1
    in_plane = target_y * LZ + target_z
    own_site = jnp.clip(target_x, 0, LX - 1) * plane_size + in_plane
    near_site = jnp.clip(target_x - LX, 0, LX - 1) * plane_size + in_plane
    next_at = jnp.roll(cluster_at, -1, axis=0)
    own_slot = jnp.take_along_axis(cluster_at, own_site.reshape(N_GX, -1), axis=1).reshape(own_site.shape)
    near_slot = clusters + jnp.take_along_axis(next_at, near_site.reshape(N_GX, -1), axis=1).reshape(near_site.shape)
    far_slot = 2 * clusters + in_plane
    second = jnp.where(target_x < LX, own_slot, jnp.where(target_x < 2 * LX, near_slot, far_slot))
    first = jnp.broadcast_to(jnp.arange(clusters, dtype=jnp.int32)[None, :, None], second.shape)
    is_self = jnp.broadcast_to((jnp.arange(CAND) == 0)[None, None, :], second.shape)
    tables = jnp.stack([first, second, image_code]).reshape(3, N_GX, clusters * CAND).astype(jnp.int32)
    return (tables, is_self.reshape(N_GX, clusters * CAND))


def draw_positions(key, part):
    site_of = cluster_sites(key)
    stretch = box_stretch(key)
    plane_size = LY * LZ
    layer_x = (site_of // plane_size)[:, :, None]
    layer_y = (site_of // LZ % LY)[:, :, None]
    layer_z = (site_of % LZ)[:, :, None]
    atom_slot = jnp.arange(8, dtype=jnp.int32)
    domain = jnp.arange(N_GX, dtype=jnp.int32)[:, None, None]
    coord_x = (domain * LX + layer_x) * 2 + atom_slot // 4
    coord_y = layer_y * 2 + atom_slot // 2 % 2
    coord_z = layer_z * 2 + atom_slot % 2
    lattice = jnp.stack([coord_x, coord_y, coord_z]).astype(jnp.float32).reshape(3, COPY_PARTICLES) + 0.5
    jitter = jax.random.uniform(jax.random.fold_in(key, 203), (3, COPY_PARTICLES), jnp.float32, -0.05, 0.05)
    return lattice * (1.0 + stretch[:, None]) + jitter


def draw_box_lengths(key, part):
    nominal = jnp.array([2.0 * LX * N_GX, 2.0 * LY, 2.0 * LZ], jnp.float32)
    return nominal * (1.0 + box_stretch(key))


def draw_velocities(key, part):
    domain = (jnp.arange(COPY_PARTICLES, dtype=jnp.int32) // ATOMS_DEV).astype(jnp.float32)
    spread = jnp.sqrt(1.0 + 2.0 * domain / (N_GX - 1))
    base = jnp.clip(jax.random.normal(jax.random.fold_in(key, 501), (3, COPY_PARTICLES), jnp.float32), -5.0, 5.0)
    return base * spread[None, :]


def draw_atom_params(key, part):
    charge = jax.random.uniform(jax.random.fold_in(key, 601), (COPY_PARTICLES,), jnp.float32, -1.0, 1.0)
    dispersion = jnp.exp(jax.random.uniform(jax.random.fold_in(key, 602), (COPY_PARTICLES,), jnp.float32, math.log(0.3), 0.0))
    repulsion = jnp.exp(jax.random.uniform(jax.random.fold_in(key, 603), (COPY_PARTICLES,), jnp.float32, math.log(0.1), math.log(0.3)))
    inverse_mass = jnp.exp(jax.random.uniform(jax.random.fold_in(key, 604), (COPY_PARTICLES,), jnp.float32, math.log(0.5), math.log(2.0)))
    return jnp.stack([charge, dispersion, repulsion, inverse_mass])


def draw_pair_list(key, part):
    tables, is_self = pair_tables(key)
    order = pair_order(key)
    return jnp.take_along_axis(tables, order[None, :, :], axis=2).reshape(3, PAIRS)


def draw_pair_count(key, part):
    return pair_counts(key)


def draw_exclusion(key, part):
    tables, is_self = pair_tables(key)
    order = pair_order(key)
    first_words = jax.random.randint(jax.random.fold_in(key, 401), (4, N_GX, PAIRS_DEV), 0, 65536)
    second_words = jax.random.randint(jax.random.fold_in(key, 402), (4, N_GX, PAIRS_DEV), 0, 65536)
    words = first_words | second_words
    upper = jnp.asarray(upper_words())[:, None, None]
    words = jnp.where(is_self[None, :, :], words & upper, words)
    return jnp.take_along_axis(words, order[None, :, :], axis=2).reshape(4, PAIRS).astype(jnp.int32)


def draw_halo_far(key, part):
    site_of = cluster_sites(key)
    cluster_at = jnp.argsort(site_of, axis=1).astype(jnp.int32)
    return cluster_at[:, :LY * LZ].reshape(N_GX * LY * LZ)


def setup_inputs(seed: int = 0, part: int = 0) -> dict:
    seeds = jax.random.split(jax.random.key(seed), 10)
    part_keys = jax.random.split(jax.random.fold_in(seeds[9], part), 10)
    return {
        "positions": draw_positions(jax.random.fold_in(jax.random.fold_in(seeds[9], part), 71), part),
        "velocities": draw_velocities(jax.random.fold_in(jax.random.fold_in(seeds[9], part), 71), part),
        "atom_params": draw_atom_params(jax.random.fold_in(jax.random.fold_in(seeds[9], part), 71), part),
        "pair_list": draw_pair_list(jax.random.fold_in(jax.random.fold_in(seeds[9], part), 71), part),
        "pair_count": draw_pair_count(jax.random.fold_in(jax.random.fold_in(seeds[9], part), 71), part),
        "exclusion": draw_exclusion(jax.random.fold_in(jax.random.fold_in(seeds[9], part), 71), part),
        "halo_far": draw_halo_far(jax.random.fold_in(jax.random.fold_in(seeds[9], part), 71), part),
        "box_lengths": draw_box_lengths(jax.random.fold_in(jax.random.fold_in(seeds[9], part), 71), part),
        "extended_variables": jnp.clip(jax.random.uniform(part_keys[8], (4,), jnp.float32, -0.3, 0.3), -0.3, 0.3),
    }


time_step = 0.25
reaction_term = 1.0 / 1331.0
thermal_scale_unit = 2.0
reservoir_inertia_mass = 4.0
barostat_gain = 0.1
pressure_target = 1.0

def pair_tiles(slot_table, pair_rows, word_rows, usable, box_lengths):
    tile_width = pair_rows.shape[1]
    first_rows = jnp.take(slot_table, pair_rows[0], axis=0).T.reshape(6, 8, tile_width)
    second_rows = jnp.take(slot_table, pair_rows[1], axis=0).T.reshape(6, 8, tile_width)
    image_y = (pair_rows[2] // 3 - 1).astype(jnp.float32) * box_lengths[1]
    image_z = (pair_rows[2] % 3 - 1).astype(jnp.float32) * box_lengths[2]
    delta_x = second_rows[0][None, :, :] - first_rows[0][:, None, :]
    delta_y = second_rows[1][None, :, :] - first_rows[1][:, None, :] + image_y
    delta_z = second_rows[2][None, :, :] - first_rows[2][:, None, :] + image_z
    shifts = (jnp.arange(64, dtype=jnp.int32) % 16)[:, None]
    mask_bits = jnp.right_shift(jnp.repeat(word_rows, 16, axis=0), shifts) & 1
    interact = (mask_bits.reshape(8, 8, tile_width) == 1) & usable[None, None, :]
    radius_sq = delta_x * delta_x + delta_y * delta_y + delta_z * delta_z
    radius_sq = jnp.where(interact, radius_sq, 1.0)
    inverse = lax.rsqrt(radius_sq)
    inverse_sq = inverse * inverse
    inverse_six = inverse_sq * inverse_sq * inverse_sq
    charge_pair = first_rows[3][:, None, :] * second_rows[3][None, :, :]
    dispersion = first_rows[4][:, None, :] * second_rows[4][None, :, :]
    repulsion = first_rows[5][:, None, :] * second_rows[5][None, :, :]
    scalar = charge_pair * (inverse * inverse_sq - reaction_term) + (12.0 * repulsion * inverse_six - 6.0 * dispersion) * inverse_six * inverse_sq
    scalar = jnp.where(interact, scalar, 0.0)
    components = (delta_x, delta_y, delta_z)
    onto_second = jnp.stack([lax.optimization_barrier(jnp.sum(scalar * component, axis=0)) for component in components])
    onto_first = -jnp.stack([lax.optimization_barrier(jnp.sum(scalar * component, axis=1)) for component in components])
    virial = -0.5 * jnp.stack([jnp.sum(scalar * component * component) for component in components])
    tile_terms = jnp.concatenate([onto_first.reshape(24, tile_width), onto_second.reshape(24, tile_width)], axis=1).T
    owners = jnp.concatenate([pair_rows[0], pair_rows[1]])
    return (tile_terms, owners, virial)

def device_forces(slot_table, pair_rows, word_rows, pair_total, box_lengths):
    slots = slot_table.shape[0]
    block_rows = PAIRS_DEV // LY
    starts = jnp.arange(LY, dtype=jnp.int32) * block_rows

    def one_block(running, first_row):
        accumulated, virial = running
        pair_block = lax.dynamic_slice_in_dim(pair_rows, first_row, block_rows, 1)
        word_block = lax.dynamic_slice_in_dim(word_rows, first_row, block_rows, 1)
        usable = first_row + jnp.arange(block_rows, dtype=jnp.int32) < pair_total
        tile_terms, owners, partial_value = pair_tiles(slot_table, pair_block, word_block, usable, box_lengths)
        accumulated = accumulated + jax.ops.segment_sum(tile_terms, owners, num_segments=slots)
        return ((accumulated, virial + partial_value), None)
    start_state = (jnp.zeros((slots, 24), jnp.float32), jnp.zeros((3,), jnp.float32))
    result, unused = lax.scan(one_block, start_state, starts)
    return result

def reference(positions, velocities, atom_params, pair_list, pair_count, exclusion, halo_far, box_lengths, extended_variables):
    clusters = LX * LY * LZ
    far_clusters = LY * LZ
    slots = 2 * clusters + far_clusters
    packed = jnp.concatenate([positions, atom_params[:3]], axis=0)
    packed = packed.reshape(6, N_GX, clusters, 8).transpose(1, 0, 2, 3)
    far_lists = halo_far.reshape(N_GX, far_clusters)
    far_rows = jax.vmap(lambda block_data, chosen: block_data[:, chosen, :])(packed, far_lists)
    domain = jnp.arange(N_GX, dtype=jnp.int32)
    near_rows = jnp.roll(packed, -1, axis=0)
    far_in = jnp.roll(far_rows, -2, axis=0)
    near_lift = jnp.where(domain == N_GX - 1, box_lengths[0], 0.0)
    far_lift = jnp.where(domain >= N_GX - 2, box_lengths[0], 0.0)
    near_rows = near_rows.at[:, 0].add(near_lift[:, None, None])
    far_in = far_in.at[:, 0].add(far_lift[:, None, None])
    tables = jnp.concatenate([packed, near_rows, far_in], axis=2)
    tables = tables.transpose(0, 2, 1, 3).reshape(N_GX, slots, 48)
    pair_blocks = pair_list.reshape(3, N_GX, PAIRS_DEV).transpose(1, 0, 2)
    word_blocks = exclusion.reshape(4, N_GX, PAIRS_DEV).transpose(1, 0, 2)

    def per_domain(item):
        return device_forces(item[0], item[1], item[2], item[3], box_lengths)
    accumulated, virials = lax.map(per_domain, (tables, pair_blocks, word_blocks, pair_count))
    own_part = accumulated[:, :clusters]
    near_back = jnp.roll(accumulated[:, clusters:2 * clusters], 1, axis=0)
    far_back = jnp.roll(accumulated[:, 2 * clusters:], 2, axis=0)
    summed = own_part + near_back
    summed = jax.vmap(lambda block_data, chosen, extra: block_data.at[chosen].add(extra))(summed, far_lists, far_back)
    forces = summed.reshape(N_GX, clusters, 3, 8).transpose(2, 0, 1, 3).reshape(3, COPY_PARTICLES)
    inverse_mass = atom_params[3]
    kinetic = 0.5 * lax.optimization_barrier(jnp.sum(velocities * velocities / inverse_mass[None, :], axis=1))
    virial = lax.optimization_barrier(jnp.sum(virials, axis=0))
    overall_motion_work = jnp.sum(kinetic)
    volume = box_lengths[0] * box_lengths[1] * box_lengths[2]
    thermal_ratio_value = 2.0 * overall_motion_work / (3.0 * COPY_PARTICLES * thermal_scale_unit)
    reservoir_damping = extended_variables[0] + reservoir_inertia_mass * (thermal_ratio_value - 1.0)
    box_rates = extended_variables[1:] + barostat_gain * (kinetic - virial - pressure_target * volume / 2.0) / (overall_motion_work / 3.0)
    new_velocities = velocities + time_step * (forces * inverse_mass[None, :] - (reservoir_damping + box_rates[:, None]) * velocities)
    new_positions = positions * (1.0 + time_step * box_rates[:, None]) + time_step * new_velocities
    new_coupling = jnp.concatenate([reservoir_damping[None], box_rates])
    return (forces, new_velocities, new_positions, new_coupling)
```

```python
import functools

import jax
import jax.numpy as jnp
from jax import lax
from jax.experimental import pallas as pl
from jax.experimental.pallas import tpu as pltpu
from jax.sharding import PartitionSpec as P

RT = 1.0 / 1331.0
L = 128
F32, BF16, I16, I32 = jnp.float32, jnp.bfloat16, jnp.int16, jnp.int32


def take(x, idx):
    dn = lax.GatherDimensionNumbers(offset_dims=(), collapsed_slice_dims=(1,), start_index_map=(1,),
                                    operand_batching_dims=(0,), start_indices_batching_dims=(0,))
    return lax.gather(x, idx[:, :, None], dn, (1, 1), mode=lax.GatherScatterMode.PROMISE_IN_BOUNDS)


def iota(shape, dim):
    return lax.broadcasted_iota(I32, shape, dim)


def to_cluster_rows(row, clusters):
    lane, sub = iota((8, L), 1), iota((8, L), 0)
    idx = 8 * (lane % 16) + sub
    part = lane // 16
    tiles = []
    for t in range((clusters + L - 1) // L):
        out = None
        for u in range(8):
            start = (8 * t + u) * L
            if start >= 8 * clusters:
                break
            got = take(row(start), idx)
            out = got if out is None else jnp.where(part == u, got, out)
        tiles.append(out)
    return tiles


def pair_kernel(count_ref, box_ref, lift_ref, halo_ref, pos_ref, par_ref, npos_ref, npar_ref, fpos_ref, fpar_ref,
                pl_ref, ex_ref, own_ref, near_ref, far_ref, vir_ref,
                tab_i, tab_j, jd, oh_j, oh_i, t_j, t_i, acc_j, acc_i, vacc):
    clusters = pos_ref.shape[1] // 8
    fars = halo_ref.shape[1]
    width = oh_j.shape[1]
    box = [box_ref[c] for c in range(3)]

    def row_of(pref, qref, c, lift):
        def row(start):
            if c < 3:
                r = pref[pl.ds(c, 1), pl.ds(start, L)]
                if c == 0 and lift is not None:
                    r = r + lift
            else:
                r = qref[pl.ds(c - 3, 1), pl.ds(start, L)]
            return jnp.broadcast_to(r, (8, L))
        return row

    tab_j[...] = jnp.zeros_like(tab_j)
    lane8 = iota((8, L), 1)
    for c in range(6):
        scale = (1.0, 1.0, 1.0, 1.0, 6.0, 12.0)[c]
        own = to_cluster_rows(row_of(pos_ref, par_ref, c, None), clusters)
        near = to_cluster_rows(row_of(npos_ref, npar_ref, c, lift_ref[0]), clusters)
        far = to_cluster_rows(row_of(fpos_ref, fpar_ref, c, lift_ref[1]), clusters)
        for t in range(2):
            tab_i[c, :, t * L:(t + 1) * L] = own[t] * scale if scale != 1.0 else own[t]
        half = clusters - L
        hal = jnp.broadcast_to(halo_ref[...], (8, fars))
        hal = jnp.concatenate([hal, jnp.zeros((8, L - fars), I32)], axis=1)
        fr = jnp.where(hal >= L, take(far[1], hal & (L - 1)), take(far[0], hal & (L - 1)))
        tab_j[c, :, 0:L] = own[0]
        rot0 = pltpu.roll(near[0], half, 1)
        rot1 = pltpu.roll(near[1], half, 1)
        tab_j[c, :, L:2 * L] = jnp.where(lane8 < half, own[1], rot0)
        tab_j[c, :, 2 * L:3 * L] = jnp.where(lane8 < half, rot0, rot1)
        tab_j[c, :, 3 * L:4 * L] = fr
    acc_j[...] = jnp.zeros_like(acc_j)
    acc_i[...] = jnp.zeros_like(acc_i)
    vacc[...] = jnp.zeros_like(vacc)

    sub = iota((8, L), 0)
    count = count_ref[0]
    shift0 = 8 * (sub % 2)
    bits = [jnp.left_shift(1, shift0 + ((sub + m) & 7)) for m in range(8)]
    base16 = iota((16, L), 0).astype(I16)
    one16 = jnp.ones((16, L), BF16)
    zero16 = jnp.zeros((16, L), BF16)

    def sub_chunk(g, first):
        cols = pl.ds(pl.multiple_of(first, L), L)
        here = slice(g * L, (g + 1) * L)
        ib = jnp.broadcast_to(pl_ref[pl.ds(0, 1), cols], (8, L))
        jb = jnp.broadcast_to(pl_ref[pl.ds(1, 1), cols], (8, L))
        sb = jnp.broadcast_to(pl_ref[pl.ds(2, 1), cols], (8, L))
        usable = lane8 < count - first
        w = [jnp.broadcast_to(ex_ref[pl.ds(k, 1), cols], (8, L)) for k in range(4)]
        words = jnp.where(sub < 4, jnp.where(sub < 2, w[0], w[1]), jnp.where(sub < 6, w[2], w[3]))
        words = jnp.where(usable, words, 0)
        il, ih = ib & (L - 1), ib >= L
        first_rows = [jnp.where(ih, take(tab_i[c, :, L:2 * L], il), take(tab_i[c, :, 0:L], il)) for c in range(6)]
        jl, jh, jm = jb & (L - 1), jb >= 2 * L, (jb & L) != 0
        second = []
        for c in range(6):
            q = [take(tab_j[c, :, t * L:(t + 1) * L], jl) for t in range(4)]
            second.append(jnp.where(jh, jnp.where(jm, q[3], q[2]), jnp.where(jm, q[1], q[0])))
        hi_y = jnp.where(sb >= 6, box[1], 0.0)
        lo_y = jnp.where(sb < 3, box[1], 0.0)
        s3 = sb - jnp.where(sb >= 6, 6, jnp.where(sb >= 3, 3, 0))
        hi_z = jnp.where(s3 == 2, box[2], 0.0)
        lo_z = jnp.where(s3 == 0, box[2], 0.0)
        xi, yi, zi, qi, ei, bi = first_rows
        yi, zi = yi - hi_y, zi - hi_z
        second[1] = second[1] - lo_y
        second[2] = second[2] - lo_z
        for c in range(6):
            jd[g, c, 0:8, :] = second[c]
            jd[g, c, 8:16, :] = second[c]
        fi, fj = [None] * 3, [None] * 3
        for m in range(7, -1, -1):
            xj, yj, zj, qj, ej, bj = [jd[g, c, m:m + 8, :] for c in range(6)] if m else second
            d = (xj - xi, yj - yi, zj - zi)
            r2 = d[0] * d[0] + d[1] * d[1] + d[2] * d[2]
            inv = lax.rsqrt(r2)
            inv2 = inv * inv
            inv6 = inv2 * inv2 * inv2
            s = qi * qj * (inv * inv2 - RT) + (bi * bj * inv6 - ei * ej) * (inv6 * inv2)
            s = jnp.where((words & bits[m]) != 0, s, 0.0)
            for c in range(3):
                f = s * d[c]
                fi[c] = f if fi[c] is None else fi[c] + f
                fj[c] = f if fj[c] is None else pltpu.roll(fj[c], 1, 0) + f
        origins = [jnp.broadcast_to(v[0:1, :], (8, L)) for v in (xi, yi, zi)]
        for c, v in enumerate((xi, yi, zi)):
            vacc[c] += fj[c] * (second[c] - origins[c]) - fi[c] * (v - origins[c])
        def split(fs):
            hi = [f.astype(BF16).astype(F32) for f in fs]
            lo = [f - h for f, h in zip(fs, hi)]
            return jnp.concatenate(hi + lo, axis=0).astype(BF16)
        tj = split(fj)
        j16 = jnp.broadcast_to(jb[0:1], (16, L)).astype(I16)
        i16 = jnp.broadcast_to(ib[0:1], (16, L)).astype(I16)
        upper = j16 >= 256
        for r in range(3):
            part = tj[16 * r:16 * r + 16]
            t_j[16 * r:16 * r + 16, here] = jnp.where(upper, zero16, part)
            t_j[48 + 16 * r:64 + 16 * r, here] = jnp.where(upper, part, zero16)
        t_i[:, here] = split(fi)
        j16 = j16 & 255
        for r in range(16):
            oh_j[16 * r:16 * r + 16, here] = jnp.where(base16 == j16 - 16 * r, one16, zero16)
        for r in range(clusters // 16):
            oh_i[16 * r:16 * r + 16, here] = jnp.where(base16 == i16 - 16 * r, one16, zero16)

    def step(b, carry):
        for g in range(width // L):
            sub_chunk(g, b * width + g * L)
        contract = (((1,), (1,)), ((), ()))
        acc_j[...] += lax.dot_general(t_j[...], oh_j[...], contract, preferred_element_type=F32)
        acc_i[...] += lax.dot_general(t_i[...], oh_i[...], contract, preferred_element_type=F32)
        return carry

    lax.fori_loop(0, (count + width - 1) // width, step, 0)

    fi = acc_i[0:24] + acc_i[24:48]
    fi = jnp.concatenate([fi, jnp.zeros((24, 2 * L - clusters), F32)], axis=1)
    lo_f = acc_j[0:24] + acc_j[24:48]
    hi_f = acc_j[48:72] + acc_j[72:96]
    tiles = [lo_f[:, 0:L], lo_f[:, L:], hi_f[:, 0:L], hi_f[:, L:]]
    hal = jnp.concatenate([halo_ref[...], jnp.full((1, L - fars), 4 * L, I32)], axis=1)
    oh_far = (jnp.broadcast_to(hal, (clusters, L)) == iota((clusters, L), 0)).astype(F32).astype(BF16)
    ff = tiles[3]
    f1 = ff.astype(BF16)
    r1 = ff - f1.astype(F32)
    f2 = r1.astype(BF16)
    f3 = (r1 - f2.astype(F32)).astype(BF16)
    far = sum(lax.dot_general(f, oh_far, (((1,), (1,)), ((), ())), preferred_element_type=F32) for f in (f3, f2, f1))
    far = jnp.concatenate([far, jnp.zeros((24, 2 * L - clusters), F32)], axis=1)
    far = [far[:, 0:L], far[:, L:]]
    pick = sub == (lane8 & 7)

    def atom_order(src, base, c, t, ref, minus=None):
        slot = base + 16 * t
        idx = (slot % L) + lane8 // 8
        got = take(src[slot // L][8 * c:8 * c + 8], idx)
        if minus is not None:
            got = got - take(minus[(16 * t) // L][8 * c:8 * c + 8], (16 * t) % L + lane8 // 8)
        ref[c:c + 1, t * L:(t + 1) * L] = jnp.sum(jnp.where(pick, got, 0.0), axis=0, keepdims=True)

    mi = [fi[:, 0:L], fi[:, L:]]
    for c in range(3):
        for t in range(clusters // 16):
            atom_order(tiles, 0, c, t, own_ref, mi)
            atom_order(tiles, clusters, c, t, near_ref)
            atom_order(far, 0, c, t, far_ref)
    for c in range(3):
        vir_ref[c:c + 1, :] = jnp.sum(vacc[c], axis=0, keepdims=True)


def pair_forces(count, box, lifts, halo, pos, par, npos, npar, fpos, fpar, pairs, words, width=512):
    smem = pl.BlockSpec(memory_space=pltpu.SMEM)
    vmem = pl.BlockSpec(memory_space=pltpu.VMEM)
    atoms = pos.shape[1]
    clusters = atoms // 8
    out = jax.ShapeDtypeStruct((3, atoms), F32)
    return pl.pallas_call(
        pair_kernel,
        out_shape=(out, out, out, jax.ShapeDtypeStruct((3, L), F32)),
        in_specs=[smem] * 3 + [vmem] * 9,
        out_specs=(vmem,) * 4,
        scratch_shapes=[
            pltpu.VMEM((6, 8, 2 * L), F32),
            pltpu.VMEM((6, 8, 4 * L), F32),
            pltpu.VMEM((width // L, 6, 16, L), F32),
            pltpu.VMEM((256, width), BF16),
            pltpu.VMEM((clusters, width), BF16),
            pltpu.VMEM((96, width), BF16),
            pltpu.VMEM((48, width), BF16),
            pltpu.VMEM((96, 256), F32),
            pltpu.VMEM((48, clusters), F32),
            pltpu.VMEM((3, 8, L), F32),
        ],
        name="pair_forces",
    )(count, box, lifts, halo, pos, par, npos, npar, fpos, fpar, pairs, words)


time_step = 0.25
thermal_scale_unit = 2.0
reservoir_inertia_mass = 4.0
barostat_gain = 0.1
pressure_target = 1.0


def passed_along(value, axis, steps):
    count = lax.axis_size(axis)
    pairs = [(source, (source + steps) % count) for source in range(count)]
    return lax.ppermute(value, axis, pairs)


def on_device(
    positions,
    velocities,
    atom_params,
    pair_list,
    pair_count,
    exclusion,
    halo_far,
    box_lengths,
    extended_variables,
):
    atoms_here = positions.shape[1]
    index, count = lax.axis_index("gx"), lax.axis_size("gx")
    inverse_mass = atom_params[3]
    kinetic = 0.5 * jnp.sum(velocities * velocities / inverse_mass[None, :], axis=1)
    packed = jnp.concatenate([positions, atom_params], axis=0)
    near_in = passed_along(packed, "gx", -1)
    far_in = passed_along(packed, "gx", -2)
    halo_in = passed_along(halo_far, "gx", -2)
    lifts = jnp.where(jnp.stack([index + 1, index + 2]) >= count, box_lengths[0], 0.0)
    own, near, far, virial = pair_forces(
        pair_count, box_lengths, lifts, halo_in[None], positions, atom_params,
        near_in[:3], near_in[3:], far_in[:3], far_in[3:], pair_list, exclusion,
    )
    virial = -0.5 * jnp.sum(virial, axis=1)
    forces = own + passed_along(near, "gx", 1) + passed_along(far, "gx", 2)
    sums = lax.psum(jnp.stack([kinetic, virial]), "gx")
    kinetic, virial = sums[0], sums[1]
    total = jnp.sum(kinetic)
    volume = box_lengths[0] * box_lengths[1] * box_lengths[2]
    ratio = 2.0 * total / (3.0 * (atoms_here * count) * thermal_scale_unit)
    damping = extended_variables[0] + reservoir_inertia_mass * (ratio - 1.0)
    box_rates = extended_variables[1:] + barostat_gain * (
        kinetic - virial - pressure_target * volume / 2.0
    ) / (total / 3.0)
    new_velocities = velocities + time_step * (
        forces * inverse_mass[None, :] - (damping + box_rates[:, None]) * velocities
    )
    new_positions = positions * (1.0 + time_step * box_rates[:, None]) + time_step * new_velocities
    return forces, new_velocities, new_positions, jnp.concatenate([damping[None], box_rates])


def solution(mesh):
    whole = ("rep", "gx")
    rows, flat = P(None, whole), P(whole)
    return jax.shard_map(
        on_device,
        mesh=mesh,
        in_specs=(rows, rows, rows, rows, flat, rows, flat, P("rep"), P("rep")),
        out_specs=(rows, rows, rows, P("rep")),
        check_vma=False,
    )
```

```python
import functools

import jax
import jax.numpy as jnp
from jax import lax
from jax.experimental import pallas as pl
from jax.experimental.pallas import tpu as pltpu
from jax.sharding import PartitionSpec as P

PLANE = 8
WIDTH = 512
MESH = pl.DeviceIdType.MESH

time_step = 0.25
thermal_scale_unit = 2.0
reservoir_inertia_mass = 4.0
barostat_gain = 0.1
pressure_target = 1.0

RT = 1.0 / 1331.0
L = 128
F32, BF16, I16, I32 = jnp.float32, jnp.bfloat16, jnp.int16, jnp.int32


def take(x, idx):
    dn = lax.GatherDimensionNumbers(offset_dims=(), collapsed_slice_dims=(1,), start_index_map=(1,),
                                    operand_batching_dims=(0,), start_indices_batching_dims=(0,))
    return lax.gather(x, idx[:, :, None], dn, (1, 1), mode=lax.GatherScatterMode.PROMISE_IN_BOUNDS)


def iota(shape, dim):
    return lax.broadcasted_iota(I32, shape, dim)


def to_cluster_rows(row, clusters):
    lane, sub = iota((8, L), 1), iota((8, L), 0)
    idx = 8 * (lane % 16) + sub
    part = lane // 16
    tiles = []
    for t in range((clusters + L - 1) // L):
        out = None
        for u in range(8):
            start = (8 * t + u) * L
            if start >= 8 * clusters:
                break
            got = take(row(start), idx)
            out = got if out is None else jnp.where(part == u, got, out)
        tiles.append(out)
    return tiles


def step_kernel(
    domains, count_ref, box_ref, ext_ref, halo_ref, pos_ref, vel_ref, par_ref, pl_ref, ex_ref,
    force_ref, nvel_ref, npos_out, coup_ref,
    npos_ref, npar_ref, fpos_ref, fpar_ref, fhalo_ref, near_ref, far_ref, near_in, far_in,
    part, src1, src2, sum1, sum2,
    tab_i, tab_j, jd, ri, wd, fs, acc_j, acc_i, vacc,
    halo_send, halo_recv, force_send, force_recv, send1, recv1, send2, recv2,
):
    planes = domains // PLANE
    me = lax.axis_index("gx")
    place, plane = lax.rem(me, PLANE), lax.div(me, PLANE)
    at = lambda shift: lax.rem(me + domains + shift, domains)
    mates = [plane * PLANE + lax.rem(place + k, PLANE) for k in range(1, PLANE)]
    columns = [lax.rem(plane + k, planes) * PLANE + place for k in range(1, planes)]

    barrier = pltpu.get_barrier_semaphore()
    greeted = [at(-1), at(-2), at(1), at(2)] + mates + columns
    for other in greeted:
        pl.semaphore_signal(barrier, inc=1, device_id={"gx": other}, device_id_type=MESH)

    def copy(src, dst, send, recv, other):
        return pltpu.make_async_remote_copy(
            src_ref=src, dst_ref=dst, send_sem=send, recv_sem=recv, device_id={"gx": other}, device_id_type=MESH
        )

    halo_copies = [
        copy(pos_ref, npos_ref, halo_send.at[0], halo_recv.at[0], at(-1)),
        copy(par_ref, npar_ref, halo_send.at[1], halo_recv.at[1], at(-1)),
        copy(pos_ref, fpos_ref, halo_send.at[2], halo_recv.at[2], at(-2)),
        copy(par_ref, fpar_ref, halo_send.at[3], halo_recv.at[3], at(-2)),
        copy(halo_ref, fhalo_ref, halo_send.at[4], halo_recv.at[4], at(-2)),
    ]
    clusters = pos_ref.shape[1] // 8
    fars = fhalo_ref.shape[1]
    width = fs.shape[0] * L
    box = [box_ref[c] for c in range(3)]

    def row_of(pref, qref, c, lift):
        def row(start):
            if c < 3:
                r = pref[pl.ds(c, 1), pl.ds(start, L)]
                if c == 0 and lift is not None:
                    r = r + lift
            else:
                r = qref[pl.ds(c - 3, 1), pl.ds(start, L)]
            return jnp.broadcast_to(r, (8, L))
        return row

    lane8 = iota((8, L), 1)
    tiles_of = clusters // 16
    half = clusters - L
    scales = (1.0, 1.0, 1.0, 1.0, 6.0, 12.0)
    for c in range(6):
        own = to_cluster_rows(row_of(pos_ref, par_ref, c, None), clusters)
        for t in range(2):
            tab_i[c, :, t * L:(t + 1) * L] = own[t] * scales[c] if scales[c] != 1.0 else own[t]
            tab_j[c, :, t * L:(t + 1) * L] = own[t]
    part[...] = jnp.zeros_like(part)
    kin = None
    for t in range(tiles_of):
        cols = slice(t * L, (t + 1) * L)
        term = vel_ref[:, cols] * vel_ref[:, cols] / par_ref[3:4, cols]
        kin = term if kin is None else kin + term
    part[0:3, :] = 0.5 * kin
    acc_j[...] = jnp.zeros_like(acc_j)
    acc_i[...] = jnp.zeros_like(acc_i)
    vacc[...] = jnp.zeros_like(vacc)
    fs[...] = jnp.zeros_like(fs)

    pl.semaphore_wait(barrier, len(greeted))
    for item in halo_copies:
        item.start()
    for item in halo_copies:
        item.wait()

    lift_near = jnp.where(me + 1 >= domains, box[0], 0.0)
    lift_far = jnp.where(me + 2 >= domains, box[0], 0.0)
    hal = jnp.concatenate(
        [jnp.broadcast_to(fhalo_ref[...], (8, fars)), jnp.zeros((8, L - fars), I32)], axis=1)
    for c in range(6):
        near = to_cluster_rows(row_of(npos_ref, npar_ref, c, lift_near), clusters)
        far = to_cluster_rows(row_of(fpos_ref, fpar_ref, c, lift_far), clusters)
        rot0 = pltpu.roll(near[0], half, 1)
        rot1 = pltpu.roll(near[1], half, 1)
        tab_j[c, :, L:2 * L] = jnp.where(lane8 < half, tab_j[c, :, L:2 * L], rot0)
        tab_j[c, :, 2 * L:3 * L] = jnp.where(lane8 < half, rot0, rot1)
        tab_j[c, :, 3 * L:4 * L] = jnp.where(
            hal >= L, take(far[1], hal & (L - 1)), take(far[0], hal & (L - 1)))


    sub = iota((8, L), 0)
    count = count_ref[0]
    shift0 = 8 * (sub % 2)
    bits = [jnp.left_shift(1, shift0 + ((sub + m) & 7)) for m in range(8)]
    one16 = jnp.ones((16, L), BF16)
    zero16 = jnp.zeros((16, L), BF16)

    groups = width // L
    base16 = iota((16, L), 0).astype(I16)

    def gather(block):
        for g in range(groups):
            first = block * width + g * L
            cols = pl.ds(pl.multiple_of(first, L), L)
            ib = jnp.broadcast_to(pl_ref[pl.ds(0, 1), cols], (8, L))
            jb = jnp.broadcast_to(pl_ref[pl.ds(1, 1), cols], (8, L))
            sb = jnp.broadcast_to(pl_ref[pl.ds(2, 1), cols], (8, L))
            usable = lane8 < count - first
            w = [jnp.broadcast_to(ex_ref[pl.ds(k, 1), cols], (8, L)) for k in range(4)]
            words = jnp.where(sub < 4, jnp.where(sub < 2, w[0], w[1]), jnp.where(sub < 6, w[2], w[3]))
            wd[g] = jnp.where(usable, words, 0)
            above_y, below_y = sb >= 6, sb < 3
            s3 = sb - jnp.where(above_y, 6, jnp.where(below_y, 0, 3))
            il, ih = ib & (L - 1), ib >= L
            jl, jh, jm = jb & (L - 1), jb >= 2 * L, (jb & L) != 0
            for c in range(6):
                v = jnp.where(ih, take(tab_i[c, :, L:2 * L], il), take(tab_i[c, :, 0:L], il))
                if c in (1, 2):
                    v = v - jnp.where(above_y if c == 1 else s3 == 2, box[c], 0.0)
                ri[g, c] = v
            for c in range(6):
                q = [take(tab_j[c, :, t * L:(t + 1) * L], jl) for t in range(4)]
                v = jnp.where(jh, jnp.where(jm, q[3], q[2]), jnp.where(jm, q[1], q[0]))
                if c in (1, 2):
                    v = v - jnp.where(below_y if c == 1 else s3 == 0, box[c], 0.0)
                jd[g, c, 0:8, :] = v
                jd[g, c, 8:16, :] = v

    def split(fs):
        hi = [f.astype(BF16).astype(F32) for f in fs]
        lo = [f - h for f, h in zip(fs, hi)]
        return jnp.concatenate(hi + lo, axis=0).astype(BF16)

    def compute(block):
        for g in range(groups):
            xi, yi, zi, qi, ei, bi = [ri[g, c] for c in range(6)]
            words = wd[g]
            fi, fj = [None] * 3, [None] * 3
            for m in range(7, -1, -1):
                xj, yj, zj, qj, ej, bj = [jd[g, c, m:m + 8, :] for c in range(6)]
                d = (xj - xi, yj - yi, zj - zi)
                r2 = d[0] * d[0] + d[1] * d[1] + d[2] * d[2]
                inv = lax.rsqrt(r2)
                inv2 = inv * inv
                inv3 = inv * inv2
                inv6 = inv3 * inv3
                s = qi * qj * (inv3 - RT) + (bi * bj * inv6 - ei * ej) * (inv6 * inv2)
                s = jnp.where((words & bits[m]) != 0, s, 0.0)
                for c in range(3):
                    f = s * d[c]
                    fi[c] = f if fi[c] is None else fi[c] + f
                    fj[c] = f if fj[c] is None else pltpu.roll(fj[c], 1, 0) + f
            for c, v in enumerate((xi, yi, zi)):
                origin = jnp.broadcast_to(ri[g, c, 0:1, :], (8, L))
                vacc[c] += fj[c] * (jd[g, c, 0:8, :] - origin) - fi[c] * (v - origin)
            for c in range(3):
                fs[g, c] = fj[c]
                fs[g, 3 + c] = fi[c]

    half_c = clusters // 2

    def dots(block):
        tjs, tis, ojs, ois = [], [], [], []
        for g in range(groups):
            cols = pl.ds(pl.multiple_of(block * width + g * L, L), L)
            j16 = jnp.broadcast_to(pl_ref[pl.ds(1, 1), cols], (16, L)).astype(I16)
            i16 = jnp.broadcast_to(pl_ref[pl.ds(0, 1), cols], (16, L)).astype(I16)
            tj = split([fs[g, c] for c in range(3)])
            ti = split([fs[g, 3 + c] for c in range(3)])
            parts = lambda t: [t[16 * r:16 * r + 16] for r in range(3)]
            which = j16 & (3 * L)
            tjs.append(jnp.concatenate(
                [jnp.where(which == k * L, p, zero16) for k in range(4) for p in parts(tj)], axis=0))
            later = i16 >= half_c
            tis.append(jnp.concatenate(
                [jnp.where(later, zero16, p) for p in parts(ti)] + [jnp.where(later, p, zero16) for p in parts(ti)], axis=0))
            j16 = j16 & (L - 1)
            i16 = jnp.where(later, i16 - half_c, i16)
            ojs.append(jnp.concatenate([jnp.where(base16 == j16 - 16 * r, one16, zero16) for r in range(L // 16)], axis=0))
            ois.append(jnp.concatenate([jnp.where(base16 == i16 - 16 * r, one16, zero16) for r in range(half_c // 16)], axis=0))
        contract = (((1,), (1,)), ((), ()))
        wide = lambda xs: jnp.concatenate(xs, axis=1)
        acc_j[...] += lax.dot_general(wide(tjs), wide(ojs), contract, preferred_element_type=F32)
        acc_i[...] += lax.dot_general(wide(tis), wide(ois), contract, preferred_element_type=F32)

    blocks = pl_ref.shape[1] // width

    def step(block, carry):
        dots(jnp.maximum(block - 1, 0))
        compute(block)
        gather(jnp.minimum(block + 1, blocks - 1))
        return carry

    gather(0)
    lax.fori_loop(0, blocks, step, 0)
    dots(blocks - 1)

    pad = jnp.zeros((24, L - half_c), F32)
    mi = [acc_i[48 * k:48 * k + 24] + acc_i[48 * k + 24:48 * k + 48] for k in range(2)]
    mi = [jnp.concatenate([v, pad], axis=1) for v in mi]
    tiles = [acc_j[48 * k:48 * k + 24] + acc_j[48 * k + 24:48 * k + 48] for k in range(4)]
    hal = jnp.concatenate([fhalo_ref[...], jnp.full((1, L - fars), 4 * L, I32)], axis=1)
    oh_far = (jnp.broadcast_to(hal, (clusters, L)) == iota((clusters, L), 0)).astype(F32).astype(BF16)
    ff = tiles[3]
    f1 = ff.astype(BF16)
    r1 = ff - f1.astype(F32)
    f2 = r1.astype(BF16)
    f3 = (r1 - f2.astype(F32)).astype(BF16)
    far = sum(lax.dot_general(f, oh_far, (((1,), (1,)), ((), ())), preferred_element_type=F32) for f in (f3, f2, f1))
    far = jnp.concatenate([far, jnp.zeros((24, 2 * L - clusters), F32)], axis=1)
    far = [far[:, 0:L], far[:, L:]]
    pick = sub == (lane8 & 7)

    def atom_order(src, base, c, t, ref, minus=None):
        slot = base + 16 * t
        idx = (slot % L) + lane8 // 8
        got = take(src[slot // L][8 * c:8 * c + 8], idx)
        if minus is not None:
            mine = minus[(16 * t) // half_c][8 * c:8 * c + 8]
            got = got - take(mine, (16 * t) % half_c + lane8 // 8)
        ref[c:c + 1, t * L:(t + 1) * L] = jnp.sum(jnp.where(pick, got, 0.0), axis=0, keepdims=True)

    for c in range(3):
        part[3 + c:4 + c, :] = -0.5 * jnp.sum(vacc[c], axis=0, keepdims=True)
    sums = jnp.sum(part[...], axis=1, keepdims=True)
    row = jnp.sum(jnp.where(sub == lane8, jnp.broadcast_to(sums, (8, L)), 0.0), axis=0, keepdims=True)
    src1[...] = row
    sum1[place] = src1[...]
    for c in range(3):
        for t in range(tiles_of):
            atom_order(tiles, clusters, c, t, near_ref)
    plane_copies = [
        copy(src1, sum1.at[place], send1.at[k], recv1.at[place], mate) for k, mate in enumerate(mates)]
    for item in plane_copies:
        item.start()
    for c in range(3):
        for t in range(tiles_of):
            atom_order(far, 0, c, t, far_ref)
    near_copy = copy(near_ref, near_in, force_send.at[0], force_recv.at[0], at(1))
    near_copy.start()
    for c in range(3):
        for t in range(tiles_of):
            atom_order(tiles, 0, c, t, force_ref, mi)
    far_copy = copy(far_ref, far_in, force_send.at[1], force_recv.at[1], at(2))
    far_copy.start()
    for k in range(1, PLANE):
        other = lax.rem(place + k, PLANE)
        copy(src1, sum1.at[other], send1.at[k - 1], recv1.at[other], mates[k - 1]).wait_recv()
    row = sum1[0]
    for k in range(1, PLANE):
        row = row + sum1[k]
    src2[...] = row
    sum2[plane] = src2[...]
    column_copies = [
        copy(src2, sum2.at[plane], send2.at[k], recv2.at[plane], other) for k, other in enumerate(columns)]
    for item in column_copies:
        item.start()
    near_copy.wait()
    far_copy.wait()
    force_ref[...] = force_ref[...] + near_in[...] + far_in[...]
    for item in plane_copies:
        item.wait_send()
    for k in range(1, planes):
        other = lax.rem(plane + k, planes)
        copy(src2, sum2.at[other], send2.at[k - 1], recv2.at[other], columns[k - 1]).wait_recv()
    row = sum2[0]
    for k in range(1, planes):
        row = row + sum2[k]
    row = jnp.broadcast_to(row, (8, L))
    one_of = [take(row, jnp.full((8, L), c, I32)) for c in range(6)]
    total = one_of[0] + one_of[1] + one_of[2]
    volume = box[0] * box[1] * box[2]
    ratio = 2.0 * total / (3.0 * (8 * clusters * domains) * thermal_scale_unit)
    damping = ext_ref[0] + reservoir_inertia_mass * (ratio - 1.0)
    coup_ref[0] = damping[0, 0]
    for c in range(3):
        rate = ext_ref[1 + c] + barostat_gain * (
            one_of[c] - one_of[3 + c] - pressure_target * volume / 2.0
        ) / (total / 3.0)
        coup_ref[1 + c] = rate[0, 0]
        drag, grow = (damping + rate)[0:1], (1.0 + time_step * rate)[0:1]
        for t in range(tiles_of):
            cols = slice(t * L, (t + 1) * L)
            v = vel_ref[c:c + 1, cols]
            v = v + time_step * (force_ref[c:c + 1, cols] * par_ref[3:4, cols] - drag * v)
            nvel_ref[c:c + 1, cols] = v
            npos_out[c:c + 1, cols] = pos_ref[c:c + 1, cols] * grow + time_step * v
    for item in column_copies:
        item.wait_send()


def on_device(
    positions,
    velocities,
    atom_params,
    pair_list,
    pair_count,
    exclusion,
    halo_far,
    box_lengths,
    extended_variables,
):
    domains = lax.axis_size("gx")
    planes = domains // PLANE
    atoms, fars = positions.shape[1], halo_far.shape[0]
    clusters, groups = atoms // 8, WIDTH // L
    smem = pl.BlockSpec(memory_space=pltpu.SMEM)
    vmem = pl.BlockSpec(memory_space=pltpu.VMEM)
    rows = jax.ShapeDtypeStruct((3, atoms), F32)
    dma = pltpu.SemaphoreType.DMA
    return pl.pallas_call(
        functools.partial(step_kernel, domains),
        out_shape=(rows, rows, rows, jax.ShapeDtypeStruct((4,), F32)),
        in_specs=[smem] * 3 + [vmem] * 6,
        out_specs=(vmem, vmem, vmem, smem),
        scratch_shapes=[
            pltpu.VMEM((3, atoms), F32),
            pltpu.VMEM((4, atoms), F32),
            pltpu.VMEM((3, atoms), F32),
            pltpu.VMEM((4, atoms), F32),
            pltpu.VMEM((1, fars), I32),
            pltpu.VMEM((3, atoms), F32),
            pltpu.VMEM((3, atoms), F32),
            pltpu.VMEM((3, atoms), F32),
            pltpu.VMEM((3, atoms), F32),
            pltpu.VMEM((8, L), F32),
            pltpu.VMEM((1, L), F32),
            pltpu.VMEM((1, L), F32),
            pltpu.VMEM((PLANE, 1, L), F32),
            pltpu.VMEM((planes, 1, L), F32),
            pltpu.VMEM((6, 8, 2 * L), F32),
            pltpu.VMEM((6, 8, 4 * L), F32),
            pltpu.VMEM((groups, 6, 16, L), F32),
            pltpu.VMEM((groups, 6, 8, L), F32),
            pltpu.VMEM((groups, 8, L), I32),
            pltpu.VMEM((groups, 6, 8, L), F32),
            pltpu.VMEM((192, L), F32),
            pltpu.VMEM((96, clusters // 2), F32),
            pltpu.VMEM((3, 8, L), F32),
            dma((5,)),
            dma((5,)),
            dma((2,)),
            dma((2,)),
            dma((PLANE - 1,)),
            dma((PLANE,)),
            dma((planes - 1,)),
            dma((planes,)),
        ],
        compiler_params=pltpu.CompilerParams(collective_id=0, has_side_effects=True),
        name="force_step",
    )(pair_count, box_lengths, extended_variables, halo_far[None], positions, velocities, atom_params,
      pair_list, exclusion)


def solution(mesh):
    whole = ("rep", "gx")
    rows, flat = P(None, whole), P(whole)
    return jax.shard_map(
        on_device,
        mesh=mesh,
        in_specs=(rows, rows, rows, rows, flat, rows, flat, P("rep"), P("rep")),
        out_specs=(rows, rows, rows, P("rep")),
        check_vma=False,
    )
```

```python
import functools

import jax
import jax.numpy as jnp
from jax import lax
from jax.experimental import pallas as pl
from jax.experimental.pallas import tpu as pltpu
from jax.sharding import PartitionSpec as P

PLANE = 8
WIDTH = 512
MESH = pl.DeviceIdType.MESH

time_step = 0.25
thermal_scale_unit = 2.0
reservoir_inertia_mass = 4.0
barostat_gain = 0.1
pressure_target = 1.0

RT = 1.0 / 1331.0
L = 128
F32, BF16, I16, I32 = jnp.float32, jnp.bfloat16, jnp.int16, jnp.int32


def take(x, idx):
    dn = lax.GatherDimensionNumbers(offset_dims=(), collapsed_slice_dims=(1,), start_index_map=(1,),
                                    operand_batching_dims=(0,), start_indices_batching_dims=(0,))
    return lax.gather(x, idx[:, :, None], dn, (1, 1), mode=lax.GatherScatterMode.PROMISE_IN_BOUNDS)


def iota(shape, dim):
    return lax.broadcasted_iota(I32, shape, dim)


def to_cluster_rows(row, clusters):
    lane, sub = iota((8, L), 1), iota((8, L), 0)
    idx = 8 * (lane % 16) + sub
    part = lane // 16
    tiles = []
    for t in range((clusters + L - 1) // L):
        out = None
        for u in range(8):
            start = (8 * t + u) * L
            if start >= 8 * clusters:
                break
            got = take(row(start), idx)
            out = got if out is None else jnp.where(part == u, got, out)
        tiles.append(out)
    return tiles


def step_kernel(
    domains, count_in, box_in, ext_in, halo_in, pos_in, vel_in, par_in, pl_in, ex_in,
    force_ref, coef_ref,
    count_ref, box_ref, ext_ref, halo_ref, pos_ref, vel_ref, par_ref, pl_ref, ex_ref,
    npos_ref, npar_ref, far_out, far_tab, near_force, far_force, near_in, far_in,
    part, src1, src2, sum1, sum2,
    tab_i, tab_j, jd, ri, wd, fs, acc_j, acc_i, vacc,
    load_sem, halo_send, halo_recv, force_send, force_recv, send1, recv1, send2, recv2, relay,
):
    planes = domains // PLANE
    me = lax.axis_index("gx")
    place, plane = lax.rem(me, PLANE), lax.div(me, PLANE)
    at = lambda shift: lax.rem(me + domains + shift, domains)
    column = lambda shift: lax.rem(plane + planes + shift, planes) * PLANE + place
    mates = [plane * PLANE + lax.rem(place + k, PLANE) for k in range(1, PLANE)]
    columns = [column(k) for k in range(1, planes)]

    barrier = pltpu.get_barrier_semaphore()
    greeted = [at(-1), at(-2), at(1), at(2), column(-1), column(1)] + mates
    for other in greeted:
        pl.semaphore_signal(barrier, inc=1, device_id={"gx": other}, device_id_type=MESH)

    loads = [
        pltpu.make_async_copy(src, dst, load_sem.at[k])
        for k, (src, dst) in enumerate((
            (pos_in, pos_ref), (par_in, par_ref), (halo_in, halo_ref), (box_in, box_ref), (vel_in, vel_ref),
            (count_in, count_ref), (ext_in, ext_ref), (pl_in, pl_ref), (ex_in, ex_ref),
        ))
    ]
    for item in loads:
        item.start()

    def copy(src, dst, send, recv, other):
        return pltpu.make_async_remote_copy(
            src_ref=src, dst_ref=dst, send_sem=send, recv_sem=recv, device_id={"gx": other}, device_id_type=MESH
        )

    halo_copies = [
        copy(pos_ref, npos_ref, halo_send.at[0], halo_recv.at[0], at(-1)),
        copy(par_ref, npar_ref, halo_send.at[1], halo_recv.at[1], at(-1)),
        copy(far_out, far_tab, halo_send.at[2], halo_recv.at[2], at(-2)),
    ]
    for item in loads[:4]:
        item.wait()

    clusters = pos_ref.shape[1] // 8
    fars = halo_ref.shape[1]
    width = fs.shape[0] * L
    box = [box_ref[c] for c in range(3)]

    def row_of(pref, qref, c, lift):
        def row(start):
            if c < 3:
                r = pref[pl.ds(c, 1), pl.ds(start, L)]
                if c == 0 and lift is not None:
                    r = r + lift
            else:
                r = qref[pl.ds(c - 3, 1), pl.ds(start, L)]
            return jnp.broadcast_to(r, (8, L))
        return row

    lane8 = iota((8, L), 1)
    tiles_of = clusters // 16
    half = clusters - L
    scales = (1.0, 1.0, 1.0, 1.0, 6.0, 12.0)
    hal = jnp.concatenate(
        [jnp.broadcast_to(halo_ref[...], (8, fars)), jnp.zeros((8, L - fars), I32)], axis=1)
    for c in range(6):
        own = to_cluster_rows(row_of(pos_ref, par_ref, c, None), clusters)
        far_out[c] = jnp.where(hal >= L, take(own[1], hal & (L - 1)), take(own[0], hal & (L - 1)))
        for t in range(2):
            tab_i[c, :, t * L:(t + 1) * L] = own[t] * scales[c] if scales[c] != 1.0 else own[t]
            tab_j[c, :, t * L:(t + 1) * L] = own[t]
    pl.semaphore_wait(barrier, len(greeted))
    for item in (halo_copies[2], halo_copies[0], halo_copies[1]):
        item.start()

    def tell(round_, distance):
        for side in (0, 1):
            pl.semaphore_signal(
                relay.at[2 * round_ + side], inc=1,
                device_id={"gx": column(distance if side else -distance)}, device_id_type=MESH)

    def hear(round_):
        for side in (0, 1):
            pl.semaphore_wait(relay.at[2 * round_ + side], 1)

    distances = []
    while 2 ** (len(distances) + 1) < planes:
        distances.append(2 ** len(distances))
    tell(0, distances[0])

    for item in loads[4:]:
        item.wait()
    part[...] = jnp.zeros_like(part)
    kin = None
    for t in range(tiles_of):
        cols = slice(t * L, (t + 1) * L)
        term = vel_ref[:, cols] * vel_ref[:, cols] / par_ref[3:4, cols]
        kin = term if kin is None else kin + term
    part[0:3, :] = 0.5 * kin
    acc_j[...] = jnp.zeros_like(acc_j)
    acc_i[...] = jnp.zeros_like(acc_i)
    vacc[...] = jnp.zeros_like(vacc)
    fs[...] = jnp.zeros_like(fs)

    for item in halo_copies:
        item.wait()
    lift_near = jnp.where(me + 1 >= domains, box[0], 0.0)
    lift_far = jnp.where(me + 2 >= domains, box[0], 0.0)
    for c in range(6):
        near = to_cluster_rows(row_of(npos_ref, npar_ref, c, lift_near), clusters)
        rot0 = pltpu.roll(near[0], half, 1)
        rot1 = pltpu.roll(near[1], half, 1)
        tab_j[c, :, L:2 * L] = jnp.where(lane8 < half, tab_j[c, :, L:2 * L], rot0)
        tab_j[c, :, 2 * L:3 * L] = jnp.where(lane8 < half, rot0, rot1)
        tab_j[c, :, 3 * L:4 * L] = far_tab[c] + lift_far if c == 0 else far_tab[c]

    sub = iota((8, L), 0)
    count = count_ref[0]
    shift0 = 8 * (sub % 2)
    bits = [jnp.left_shift(1, shift0 + ((sub + m) & 7)) for m in range(8)]
    one16 = jnp.ones((16, L), BF16)
    zero16 = jnp.zeros((16, L), BF16)

    groups = width // L
    base16 = iota((16, L), 0).astype(I16)

    def gather(block):
        for g in range(groups):
            first = block * width + g * L
            cols = pl.ds(pl.multiple_of(first, L), L)
            ib = jnp.broadcast_to(pl_ref[pl.ds(0, 1), cols], (8, L))
            jb = jnp.broadcast_to(pl_ref[pl.ds(1, 1), cols], (8, L))
            sb = jnp.broadcast_to(pl_ref[pl.ds(2, 1), cols], (8, L))
            usable = lane8 < count - first
            w = [jnp.broadcast_to(ex_ref[pl.ds(k, 1), cols], (8, L)) for k in range(4)]
            words = jnp.where(sub < 4, jnp.where(sub < 2, w[0], w[1]), jnp.where(sub < 6, w[2], w[3]))
            wd[g] = jnp.where(usable, words, 0)
            above_y, below_y = sb >= 6, sb < 3
            s3 = sb - jnp.where(above_y, 6, jnp.where(below_y, 0, 3))
            il, ih = ib & (L - 1), ib >= L
            jl, jh, jm = jb & (L - 1), jb >= 2 * L, (jb & L) != 0
            for c in range(6):
                v = jnp.where(ih, take(tab_i[c, :, L:2 * L], il), take(tab_i[c, :, 0:L], il))
                if c in (1, 2):
                    v = v - jnp.where(above_y if c == 1 else s3 == 2, box[c], 0.0)
                ri[g, c] = v
            for c in range(6):
                q = [take(tab_j[c, :, t * L:(t + 1) * L], jl) for t in range(4)]
                v = jnp.where(jh, jnp.where(jm, q[3], q[2]), jnp.where(jm, q[1], q[0]))
                if c in (1, 2):
                    v = v - jnp.where(below_y if c == 1 else s3 == 0, box[c], 0.0)
                jd[g, c, 0:8, :] = v
                jd[g, c, 8:16, :] = v

    def split(fs):
        hi = [f.astype(BF16).astype(F32) for f in fs]
        lo = [f - h for f, h in zip(fs, hi)]
        return jnp.concatenate(hi + lo, axis=0).astype(BF16)

    def compute(block):
        for g in range(groups):
            xi, yi, zi, qi, ei, bi = [ri[g, c] for c in range(6)]
            words = wd[g]
            fi, fj = [None] * 3, [None] * 3
            for m in range(7, -1, -1):
                xj, yj, zj, qj, ej, bj = [jd[g, c, m:m + 8, :] for c in range(6)]
                d = (xj - xi, yj - yi, zj - zi)
                r2 = d[0] * d[0] + d[1] * d[1] + d[2] * d[2]
                inv = lax.rsqrt(r2)
                inv2 = inv * inv
                inv3 = inv * inv2
                inv6 = inv3 * inv3
                s = qi * qj * (inv3 - RT) + (bi * bj * inv6 - ei * ej) * (inv6 * inv2)
                s = jnp.where((words & bits[m]) != 0, s, 0.0)
                for c in range(3):
                    f = s * d[c]
                    fi[c] = f if fi[c] is None else fi[c] + f
                    fj[c] = f if fj[c] is None else pltpu.roll(fj[c], 1, 0) + f
            for c, v in enumerate((xi, yi, zi)):
                origin = jnp.broadcast_to(ri[g, c, 0:1, :], (8, L))
                vacc[c] += fj[c] * (jd[g, c, 0:8, :] - origin) - fi[c] * (v - origin)
            for c in range(3):
                fs[g, c] = fj[c]
                fs[g, 3 + c] = fi[c]

    half_c = clusters // 2

    def dots(block):
        tjs, tis, ojs, ois = [], [], [], []
        for g in range(groups):
            cols = pl.ds(pl.multiple_of(block * width + g * L, L), L)
            j16 = jnp.broadcast_to(pl_ref[pl.ds(1, 1), cols], (16, L)).astype(I16)
            i16 = jnp.broadcast_to(pl_ref[pl.ds(0, 1), cols], (16, L)).astype(I16)
            tj = split([fs[g, c] for c in range(3)])
            ti = split([fs[g, 3 + c] for c in range(3)])
            parts = lambda t: [t[16 * r:16 * r + 16] for r in range(3)]
            which = j16 & (3 * L)
            tjs.append(jnp.concatenate(
                [jnp.where(which == k * L, p, zero16) for k in range(4) for p in parts(tj)], axis=0))
            later = i16 >= half_c
            tis.append(jnp.concatenate(
                [jnp.where(later, zero16, p) for p in parts(ti)] + [jnp.where(later, p, zero16) for p in parts(ti)], axis=0))
            j16 = j16 & (L - 1)
            i16 = jnp.where(later, i16 - half_c, i16)
            ojs.append(jnp.concatenate([jnp.where(base16 == j16 - 16 * r, one16, zero16) for r in range(L // 16)], axis=0))
            ois.append(jnp.concatenate([jnp.where(base16 == i16 - 16 * r, one16, zero16) for r in range(half_c // 16)], axis=0))
        contract = (((1,), (1,)), ((), ()))
        wide = lambda xs: jnp.concatenate(xs, axis=1)
        acc_j[...] += lax.dot_general(wide(tjs), wide(ojs), contract, preferred_element_type=F32)
        acc_i[...] += lax.dot_general(wide(tis), wide(ois), contract, preferred_element_type=F32)

    blocks = pl_ref.shape[1] // width

    def step(block, carry):
        dots(jnp.maximum(block - 1, 0))
        compute(block)
        gather(jnp.minimum(block + 1, blocks - 1))
        return carry

    gather(0)
    rounds = len(distances)
    marks = [0] + [blocks - (4 + (rounds - 1 - k) * 4) for k in range(rounds)] + [blocks]
    for k in range(rounds + 1):
        lax.fori_loop(marks[k], marks[k + 1], step, 0)
        if k < rounds:
            hear(k)
            if k + 1 < rounds:
                tell(k + 1, distances[k + 1])
    dots(blocks - 1)

    for c in range(3):
        part[3 + c:4 + c, :] = -0.5 * jnp.sum(vacc[c], axis=0, keepdims=True)
    sums = jnp.sum(part[...], axis=1, keepdims=True)
    row = jnp.sum(jnp.where(sub == lane8, jnp.broadcast_to(sums, (8, L)), 0.0), axis=0, keepdims=True)
    src1[...] = row
    sum1[place] = src1[...]
    plane_copies = [
        copy(src1, sum1.at[place], send1.at[k], recv1.at[place], mate) for k, mate in enumerate(mates)]
    for item in plane_copies:
        item.start()
    tile_at = lambda k: acc_j[48 * k:48 * k + 24] + acc_j[48 * k + 24:48 * k + 48]
    near_force[0] = tile_at(1)
    near_force[1] = tile_at(2)
    far_force[...] = tile_at(3)
    tiles = [tile_at(0), near_force[0]]
    pad = jnp.zeros((24, L - half_c), F32)
    mi = [acc_i[48 * k:48 * k + 24] + acc_i[48 * k + 24:48 * k + 48] for k in range(2)]
    mi = [jnp.concatenate([v, pad], axis=1) for v in mi]
    hal1 = jnp.concatenate([halo_ref[...], jnp.full((1, L - fars), 4 * L, I32)], axis=1)
    oh_far = (jnp.broadcast_to(hal1, (clusters, L)) == iota((clusters, L), 0)).astype(F32).astype(BF16)
    near_copy = copy(near_force, near_in, force_send.at[0], force_recv.at[0], at(1))
    far_copy = copy(far_force, far_in, force_send.at[1], force_recv.at[1], at(2))
    near_copy.start()
    far_copy.start()

    for k in range(1, PLANE):
        other = lax.rem(place + k, PLANE)
        copy(src1, sum1.at[other], send1.at[k - 1], recv1.at[other], mates[k - 1]).wait_recv()
    row = sum1[0]
    for k in range(1, PLANE):
        row = row + sum1[k]
    src2[...] = row
    sum2[plane] = src2[...]
    column_copies = [
        copy(src2, sum2.at[plane], send2.at[k], recv2.at[plane], other) for k, other in enumerate(columns)]
    for item in column_copies:
        item.start()

    near_copy.wait()
    far_copy.wait()
    ff = far_in[...]
    f1 = ff.astype(BF16)
    r1 = ff - f1.astype(F32)
    f2 = r1.astype(BF16)
    f3 = (r1 - f2.astype(F32)).astype(BF16)
    far = sum(lax.dot_general(f, oh_far, (((1,), (1,)), ((), ())), preferred_element_type=F32) for f in (f3, f2, f1))
    tiles[0] = tiles[0] + far[:, 0:L]
    tiles[1] = tiles[1] + jnp.concatenate([far[:, L:], jnp.zeros((24, 2 * L - clusters), F32)], axis=1)
    back = [near_in[0], near_in[1]]
    pick = sub == (lane8 & 7)
    for c in range(3):
        for t in range(tiles_of):
            def window(tabs, slot, size):
                return take(tabs[slot // size][8 * c:8 * c + 8], slot % size + lane8 // 8)
            got = window(tiles, 16 * t, L) - window(mi, 16 * t, half_c) + window(back, half + 16 * t, L)
            force_ref[c:c + 1, t * L:(t + 1) * L] = jnp.sum(jnp.where(pick, got, 0.0), axis=0, keepdims=True)

    for item in plane_copies:
        item.wait_send()
    for k in range(1, planes):
        other = lax.rem(plane + k, planes)
        copy(src2, sum2.at[other], send2.at[k - 1], recv2.at[other], columns[k - 1]).wait_recv()
    row = sum2[0]
    for k in range(1, planes):
        row = row + sum2[k]
    row = jnp.broadcast_to(row, (8, L))
    one_of = [take(row, jnp.full((8, L), c, I32)) for c in range(6)]
    total = one_of[0] + one_of[1] + one_of[2]
    volume = box[0] * box[1] * box[2]
    ratio = 2.0 * total / (3.0 * (8 * clusters * domains) * thermal_scale_unit)
    coef = ext_ref[0] + reservoir_inertia_mass * (ratio - 1.0)
    for c in range(3):
        rate = ext_ref[1 + c] + barostat_gain * (
            one_of[c] - one_of[3 + c] - pressure_target * volume / 2.0
        ) / (total / 3.0)
        coef = jnp.where(sub == 1 + c, rate, coef)
    coef_ref[...] = coef
    for item in column_copies:
        item.wait_send()


def update_kernel(force_in, coef_ref, pos_ref, vel_ref, par_ref, force_ref, nvel_ref, npos_ref, coup_ref):
    coef = coef_ref[...]
    for k in range(4):
        coup_ref[k] = coef[k, 0]
    drag, grow = coef[0:1] + coef[1:4], 1.0 + time_step * coef[1:4]
    for t in range(pos_ref.shape[1] // L):
        cols = slice(t * L, (t + 1) * L)
        f, v = force_in[:, cols], vel_ref[:, cols]
        v = v + time_step * (f * par_ref[3:4, cols] - drag * v)
        force_ref[:, cols] = f
        nvel_ref[:, cols] = v
        npos_ref[:, cols] = pos_ref[:, cols] * grow + time_step * v


def on_device(
    positions,
    velocities,
    atom_params,
    pair_list,
    pair_count,
    exclusion,
    halo_far,
    box_lengths,
    extended_variables,
):
    domains = lax.axis_size("gx")
    planes = domains // PLANE
    atoms, fars = positions.shape[1], halo_far.shape[0]
    clusters, groups = atoms // 8, WIDTH // L
    vmem = pl.BlockSpec(memory_space=pltpu.VMEM)
    rows = jax.ShapeDtypeStruct((3, atoms), F32)
    dma = pltpu.SemaphoreType.DMA
    forces, coef = pl.pallas_call(
        functools.partial(step_kernel, domains),
        out_shape=(rows, jax.ShapeDtypeStruct((8, L), F32)),
        in_specs=[pl.BlockSpec(memory_space=pltpu.HBM)] * 9,
        out_specs=(vmem, vmem),
        scratch_shapes=[
            pltpu.SMEM((1,), I32),
            pltpu.SMEM((3,), F32),
            pltpu.SMEM((4,), F32),
            pltpu.VMEM((1, fars), I32),
            pltpu.VMEM((3, atoms), F32),
            pltpu.VMEM((3, atoms), F32),
            pltpu.VMEM((4, atoms), F32),
            pltpu.VMEM(pair_list.shape, I32),
            pltpu.VMEM(exclusion.shape, I32),
            pltpu.VMEM((3, atoms), F32),
            pltpu.VMEM((4, atoms), F32),
            pltpu.VMEM((6, 8, L), F32),
            pltpu.VMEM((6, 8, L), F32),
            pltpu.VMEM((2, 24, L), F32),
            pltpu.VMEM((24, L), F32),
            pltpu.VMEM((2, 24, L), F32),
            pltpu.VMEM((24, L), F32),
            pltpu.VMEM((8, L), F32),
            pltpu.VMEM((1, L), F32),
            pltpu.VMEM((1, L), F32),
            pltpu.VMEM((PLANE, 1, L), F32),
            pltpu.VMEM((planes, 1, L), F32),
            pltpu.VMEM((6, 8, 2 * L), F32),
            pltpu.VMEM((6, 8, 4 * L), F32),
            pltpu.VMEM((groups, 6, 16, L), F32),
            pltpu.VMEM((groups, 6, 8, L), F32),
            pltpu.VMEM((groups, 8, L), I32),
            pltpu.VMEM((groups, 6, 8, L), F32),
            pltpu.VMEM((192, L), F32),
            pltpu.VMEM((96, clusters // 2), F32),
            pltpu.VMEM((3, 8, L), F32),
            dma((9,)),
            dma((3,)),
            dma((3,)),
            dma((2,)),
            dma((2,)),
            dma((PLANE - 1,)),
            dma((PLANE,)),
            dma((planes - 1,)),
            dma((planes,)),
            pltpu.SemaphoreType.REGULAR((2 * planes.bit_length(),)),
        ],
        compiler_params=pltpu.CompilerParams(collective_id=0, has_side_effects=True),
        name="force_step",
    )(pair_count, box_lengths, extended_variables, halo_far[None], positions, velocities, atom_params,
      pair_list, exclusion)
    return pl.pallas_call(
        update_kernel,
        out_shape=(rows, rows, rows, jax.ShapeDtypeStruct((4,), F32)),
        in_specs=[vmem] * 5,
        out_specs=(vmem, vmem, vmem, pl.BlockSpec(memory_space=pltpu.SMEM)),
        name="update",
    )(forces, coef, positions, velocities, atom_params)


def solution(mesh):
    whole = ("rep", "gx")
    rows, flat = P(None, whole), P(whole)
    return jax.shard_map(
        on_device,
        mesh=mesh,
        in_specs=(rows, rows, rows, rows, flat, rows, flat, P("rep"), P("rep")),
        out_specs=(rows, rows, rows, P("rep")),
        check_vma=False,
    )
```

```python
import functools

import jax
import jax.numpy as jnp
from jax import lax
from jax.experimental import pallas as pl
from jax.experimental.pallas import tpu as pltpu
from jax.sharding import PartitionSpec as P

PLANE = 8
WIDTH = 512
MESH = pl.DeviceIdType.MESH

time_step = 0.25
thermal_scale_unit = 2.0
reservoir_inertia_mass = 4.0
barostat_gain = 0.1
pressure_target = 1.0

RT = 1.0 / 1331.0
L = 128
F32, BF16, I16, I32 = jnp.float32, jnp.bfloat16, jnp.int16, jnp.int32


def take(x, idx):
    dn = lax.GatherDimensionNumbers(offset_dims=(), collapsed_slice_dims=(1,), start_index_map=(1,),
                                    operand_batching_dims=(0,), start_indices_batching_dims=(0,))
    return lax.gather(x, idx[:, :, None], dn, (1, 1), mode=lax.GatherScatterMode.PROMISE_IN_BOUNDS)


def iota(shape, dim):
    return lax.broadcasted_iota(I32, shape, dim)


def to_cluster_rows(row, clusters):
    lane, sub = iota((8, L), 1), iota((8, L), 0)
    idx = 8 * (lane % 16) + sub
    part = lane // 16
    tiles = []
    for t in range((clusters + L - 1) // L):
        out = None
        for u in range(8):
            start = (8 * t + u) * L
            if start >= 8 * clusters:
                break
            got = take(row(start), idx)
            out = got if out is None else jnp.where(part == u, got, out)
        tiles.append(out)
    return tiles


def step_kernel(
    domains, count_in, box_in, ext_in, halo_in, pos_in, vel_in, par_in, pl_in, ex_in,
    force_ref, coef_ref,
    count_ref, box_ref, ext_ref, halo_ref, pos_ref, vel_ref, par_ref, pl_ref, ex_ref,
    npos_ref, npar_ref, far_out, far_tab, near_force, far_force, near_in, far_in,
    part, src1, src2, sum1, sum2,
    tab_i, tab_j, jd, ri, wd, fs, acc_j, acc_i, vacc,
    load_sem, halo_send, halo_recv, force_send, force_recv, send1, recv1, send2, recv2, relay,
):
    planes = domains // PLANE
    me = lax.axis_index("gx")
    place, plane = lax.rem(me, PLANE), lax.div(me, PLANE)
    at = lambda shift: lax.rem(me + domains + shift, domains)
    column = lambda shift: lax.rem(plane + planes + shift, planes) * PLANE + place
    mates = [plane * PLANE + lax.rem(place + k, PLANE) for k in range(1, PLANE)]
    steps = sorted(range(1, planes), key=lambda k: min(k, planes - k))
    columns = [column(k) for k in steps]

    barrier = pltpu.get_barrier_semaphore()
    greeted = [at(2), at(1), at(-1), at(-2), column(1), column(-1)] + mates
    for other in greeted:
        pl.semaphore_signal(barrier, inc=1, device_id={"gx": other}, device_id_type=MESH)

    loads = [
        pltpu.make_async_copy(src, dst, load_sem.at[k])
        for k, (src, dst) in enumerate((
            (pos_in, pos_ref), (par_in, par_ref), (halo_in, halo_ref), (box_in, box_ref), (vel_in, vel_ref),
            (count_in, count_ref), (ext_in, ext_ref), (pl_in, pl_ref), (ex_in, ex_ref),
        ))
    ]
    for item in loads:
        item.start()

    def copy(src, dst, send, recv, other):
        return pltpu.make_async_remote_copy(
            src_ref=src, dst_ref=dst, send_sem=send, recv_sem=recv, device_id={"gx": other}, device_id_type=MESH
        )

    halo_copies = [
        copy(pos_ref, npos_ref, halo_send.at[0], halo_recv.at[0], at(-1)),
        copy(par_ref, npar_ref, halo_send.at[1], halo_recv.at[1], at(-1)),
        copy(far_out, far_tab, halo_send.at[2], halo_recv.at[2], at(-2)),
    ]
    for item in loads[:4]:
        item.wait()

    clusters = pos_ref.shape[1] // 8
    fars = halo_ref.shape[1]
    width = fs.shape[0] * L
    box = [box_ref[c] for c in range(3)]

    def row_of(pref, qref, c, lift):
        def row(start):
            if c < 3:
                r = pref[pl.ds(c, 1), pl.ds(start, L)]
                if c == 0 and lift is not None:
                    r = r + lift
            else:
                r = qref[pl.ds(c - 3, 1), pl.ds(start, L)]
            return jnp.broadcast_to(r, (8, L))
        return row

    lane8 = iota((8, L), 1)
    tiles_of = clusters // 16
    half = clusters - L
    scales = (1.0, 1.0, 1.0, 1.0, 6.0, 12.0)
    hal = jnp.concatenate(
        [jnp.broadcast_to(halo_ref[...], (8, fars)), jnp.zeros((8, L - fars), I32)], axis=1)
    for c in range(6):
        own = to_cluster_rows(row_of(pos_ref, par_ref, c, None), clusters)
        far_out[c] = jnp.where(hal >= L, take(own[1], hal & (L - 1)), take(own[0], hal & (L - 1)))
        for t in range(2):
            tab_i[c, :, t * L:(t + 1) * L] = own[t] * scales[c] if scales[c] != 1.0 else own[t]
            tab_j[c, :, t * L:(t + 1) * L] = own[t]
    pl.semaphore_wait(barrier, len(greeted))
    for item in (halo_copies[2], halo_copies[0], halo_copies[1]):
        item.start()

    def tell(round_, distance):
        for side in (0, 1):
            pl.semaphore_signal(
                relay.at[2 * round_ + side], inc=1,
                device_id={"gx": column(distance if side else -distance)}, device_id_type=MESH)

    def hear(round_):
        for side in (0, 1):
            pl.semaphore_wait(relay.at[2 * round_ + side], 1)

    distances = []
    while 2 ** (len(distances) + 1) < planes:
        distances.append(2 ** len(distances))
    tell(0, distances[0])

    for item in loads[4:]:
        item.wait()
    part[...] = jnp.zeros_like(part)
    kin = None
    for t in range(tiles_of):
        cols = slice(t * L, (t + 1) * L)
        term = vel_ref[:, cols] * vel_ref[:, cols] / par_ref[3:4, cols]
        kin = term if kin is None else kin + term
    part[0:3, :] = 0.5 * kin
    acc_j[...] = jnp.zeros_like(acc_j)
    acc_i[...] = jnp.zeros_like(acc_i)
    vacc[...] = jnp.zeros_like(vacc)
    fs[...] = jnp.zeros_like(fs)

    for item in halo_copies:
        item.wait()
    lift_near = jnp.where(me + 1 >= domains, box[0], 0.0)
    lift_far = jnp.where(me + 2 >= domains, box[0], 0.0)
    for c in range(6):
        near = to_cluster_rows(row_of(npos_ref, npar_ref, c, lift_near), clusters)
        rot0 = pltpu.roll(near[0], half, 1)
        rot1 = pltpu.roll(near[1], half, 1)
        tab_j[c, :, L:2 * L] = jnp.where(lane8 < half, tab_j[c, :, L:2 * L], rot0)
        tab_j[c, :, 2 * L:3 * L] = jnp.where(lane8 < half, rot0, rot1)
        tab_j[c, :, 3 * L:4 * L] = far_tab[c] + lift_far if c == 0 else far_tab[c]

    sub = iota((8, L), 0)
    count = count_ref[0]
    shift0 = 8 * (sub % 2)
    bits = [jnp.left_shift(1, shift0 + ((sub + m) & 7)) for m in range(8)]
    one16 = jnp.ones((16, L), BF16)
    zero16 = jnp.zeros((16, L), BF16)

    groups = width // L
    base16 = iota((16, L), 0).astype(I16)

    def gather(block):
        for g in range(groups):
            first = block * width + g * L
            cols = pl.ds(pl.multiple_of(first, L), L)
            ib = jnp.broadcast_to(pl_ref[pl.ds(0, 1), cols], (8, L))
            jb = jnp.broadcast_to(pl_ref[pl.ds(1, 1), cols], (8, L))
            sb = jnp.broadcast_to(pl_ref[pl.ds(2, 1), cols], (8, L))
            usable = lane8 < count - first
            w = [jnp.broadcast_to(ex_ref[pl.ds(k, 1), cols], (8, L)) for k in range(4)]
            words = jnp.where(sub < 4, jnp.where(sub < 2, w[0], w[1]), jnp.where(sub < 6, w[2], w[3]))
            wd[g] = jnp.where(usable, words, 0)
            above_y, below_y = sb >= 6, sb < 3
            s3 = sb - jnp.where(above_y, 6, jnp.where(below_y, 0, 3))
            il, ih = ib & (L - 1), ib >= L
            jl, jh, jm = jb & (L - 1), jb >= 2 * L, (jb & L) != 0
            for c in range(6):
                v = jnp.where(ih, take(tab_i[c, :, L:2 * L], il), take(tab_i[c, :, 0:L], il))
                if c in (1, 2):
                    v = v - jnp.where(above_y if c == 1 else s3 == 2, box[c], 0.0)
                ri[g, c] = v
            for c in range(6):
                q = [take(tab_j[c, :, t * L:(t + 1) * L], jl) for t in range(4)]
                v = jnp.where(jh, jnp.where(jm, q[3], q[2]), jnp.where(jm, q[1], q[0]))
                if c in (1, 2):
                    v = v - jnp.where(below_y if c == 1 else s3 == 0, box[c], 0.0)
                jd[g, c, 0:8, :] = v
                jd[g, c, 8:16, :] = v

    def split(fs):
        hi = [f.astype(BF16).astype(F32) for f in fs]
        lo = [f - h for f, h in zip(fs, hi)]
        return jnp.concatenate(hi + lo, axis=0).astype(BF16)

    def compute(block):
        for g in range(groups):
            xi, yi, zi, qi, ei, bi = [ri[g, c] for c in range(6)]
            words = wd[g]
            fi, fj = [None] * 3, [None] * 3
            for m in range(7, -1, -1):
                xj, yj, zj, qj, ej, bj = [jd[g, c, m:m + 8, :] for c in range(6)]
                d = (xj - xi, yj - yi, zj - zi)
                r2 = d[0] * d[0] + d[1] * d[1] + d[2] * d[2]
                inv = lax.rsqrt(r2)
                inv2 = inv * inv
                inv3 = inv * inv2
                inv6 = inv3 * inv3
                s = qi * qj * (inv3 - RT) + (bi * bj * inv6 - ei * ej) * (inv6 * inv2)
                s = jnp.where((words & bits[m]) != 0, s, 0.0)
                for c in range(3):
                    f = s * d[c]
                    fi[c] = f if fi[c] is None else fi[c] + f
                    fj[c] = f if fj[c] is None else pltpu.roll(fj[c], 1, 0) + f
            for c, v in enumerate((xi, yi, zi)):
                origin = jnp.broadcast_to(ri[g, c, 0:1, :], (8, L))
                vacc[c] += fj[c] * (jd[g, c, 0:8, :] - origin) - fi[c] * (v - origin)
            for c in range(3):
                fs[g, c] = fj[c]
                fs[g, 3 + c] = fi[c]

    half_c = clusters // 2

    def dots(block):
        tjs, tis, ojs, ois = [], [], [], []
        for g in range(groups):
            cols = pl.ds(pl.multiple_of(block * width + g * L, L), L)
            j16 = jnp.broadcast_to(pl_ref[pl.ds(1, 1), cols], (16, L)).astype(I16)
            i16 = jnp.broadcast_to(pl_ref[pl.ds(0, 1), cols], (16, L)).astype(I16)
            tj = split([fs[g, c] for c in range(3)])
            ti = split([fs[g, 3 + c] for c in range(3)])
            parts = lambda t: [t[16 * r:16 * r + 16] for r in range(3)]
            which = j16 & (3 * L)
            tjs.append(jnp.concatenate(
                [jnp.where(which == k * L, p, zero16) for k in range(4) for p in parts(tj)], axis=0))
            later = i16 >= half_c
            tis.append(jnp.concatenate(
                [jnp.where(later, zero16, p) for p in parts(ti)] + [jnp.where(later, p, zero16) for p in parts(ti)], axis=0))
            j16 = j16 & (L - 1)
            i16 = jnp.where(later, i16 - half_c, i16)
            ojs.append(jnp.concatenate([jnp.where(base16 == j16 - 16 * r, one16, zero16) for r in range(L // 16)], axis=0))
            ois.append(jnp.concatenate([jnp.where(base16 == i16 - 16 * r, one16, zero16) for r in range(half_c // 16)], axis=0))
        contract = (((1,), (1,)), ((), ()))
        wide = lambda xs: jnp.concatenate(xs, axis=1)
        acc_j[...] += lax.dot_general(wide(tjs), wide(ojs), contract, preferred_element_type=F32)
        acc_i[...] += lax.dot_general(wide(tis), wide(ois), contract, preferred_element_type=F32)

    blocks = pl_ref.shape[1] // width

    def step(block, carry):
        dots(jnp.maximum(block - 1, 0))
        compute(block)
        gather(jnp.minimum(block + 1, blocks - 1))
        return carry

    gather(0)
    rounds = len(distances)
    marks = [0] + [5 + 7 * k for k in range(rounds - 1)] + [blocks]
    for k in range(rounds):
        lax.fori_loop(marks[k], marks[k + 1], step, 0)
        if k + 1 < rounds:
            hear(k)
            tell(k + 1, distances[k + 1])
    dots(blocks - 1)

    for c in range(3):
        part[3 + c:4 + c, :] = -0.5 * jnp.sum(vacc[c], axis=0, keepdims=True)
    sums = jnp.sum(part[...], axis=1, keepdims=True)
    row = jnp.sum(jnp.where(sub == lane8, jnp.broadcast_to(sums, (8, L)), 0.0), axis=0, keepdims=True)
    src1[...] = row
    sum1[place] = src1[...]
    plane_copies = [
        copy(src1, sum1.at[place], send1.at[k], recv1.at[place], mate) for k, mate in enumerate(mates)]
    for item in plane_copies:
        item.start()
    tile_at = lambda k: acc_j[48 * k:48 * k + 24] + acc_j[48 * k + 24:48 * k + 48]
    near_force[0] = tile_at(1)
    near_force[1] = tile_at(2)
    far_force[...] = tile_at(3)
    tiles = [tile_at(0), near_force[0]]
    pad = jnp.zeros((24, L - half_c), F32)
    mi = [acc_i[48 * k:48 * k + 24] + acc_i[48 * k + 24:48 * k + 48] for k in range(2)]
    mi = [jnp.concatenate([v, pad], axis=1) for v in mi]
    hal1 = jnp.concatenate([halo_ref[...], jnp.full((1, L - fars), 4 * L, I32)], axis=1)
    oh_far = (jnp.broadcast_to(hal1, (clusters, L)) == iota((clusters, L), 0)).astype(F32).astype(BF16)
    near_copy = copy(near_force, near_in, force_send.at[0], force_recv.at[0], at(1))
    far_copy = copy(far_force, far_in, force_send.at[1], force_recv.at[1], at(2))
    near_copy.start()
    far_copy.start()

    hear(rounds - 1)
    for k in range(1, PLANE):
        other = lax.rem(place + k, PLANE)
        copy(src1, sum1.at[other], send1.at[k - 1], recv1.at[other], mates[k - 1]).wait_recv()
    row = sum1[0]
    for k in range(1, PLANE):
        row = row + sum1[k]
    src2[...] = row
    sum2[plane] = src2[...]
    column_copies = [
        copy(src2, sum2.at[plane], send2.at[k], recv2.at[plane], other) for k, other in enumerate(columns)]
    for item in column_copies:
        item.start()

    near_copy.wait()
    far_copy.wait()
    ff = far_in[...]
    f1 = ff.astype(BF16)
    r1 = ff - f1.astype(F32)
    f2 = r1.astype(BF16)
    f3 = (r1 - f2.astype(F32)).astype(BF16)
    far = sum(lax.dot_general(f, oh_far, (((1,), (1,)), ((), ())), preferred_element_type=F32) for f in (f3, f2, f1))
    tiles[0] = tiles[0] + far[:, 0:L]
    tiles[1] = tiles[1] + jnp.concatenate([far[:, L:], jnp.zeros((24, 2 * L - clusters), F32)], axis=1)
    back = [near_in[0], near_in[1]]
    pick = sub == (lane8 & 7)
    for c in range(3):
        for t in range(tiles_of):
            def window(tabs, slot, size):
                return take(tabs[slot // size][8 * c:8 * c + 8], slot % size + lane8 // 8)
            got = window(tiles, 16 * t, L) - window(mi, 16 * t, half_c) + window(back, half + 16 * t, L)
            force_ref[c:c + 1, t * L:(t + 1) * L] = jnp.sum(jnp.where(pick, got, 0.0), axis=0, keepdims=True)

    for item in plane_copies:
        item.wait_send()
    for k, step_ in enumerate(steps):
        other = lax.rem(plane + step_, planes)
        copy(src2, sum2.at[other], send2.at[k], recv2.at[other], columns[k]).wait_recv()
    row = sum2[0]
    for k in range(1, planes):
        row = row + sum2[k]
    row = jnp.broadcast_to(row, (8, L))
    one_of = [take(row, jnp.full((8, L), c, I32)) for c in range(6)]
    total = one_of[0] + one_of[1] + one_of[2]
    volume = box[0] * box[1] * box[2]
    ratio = 2.0 * total / (3.0 * (8 * clusters * domains) * thermal_scale_unit)
    coef = ext_ref[0] + reservoir_inertia_mass * (ratio - 1.0)
    for c in range(3):
        rate = ext_ref[1 + c] + barostat_gain * (
            one_of[c] - one_of[3 + c] - pressure_target * volume / 2.0
        ) / (total / 3.0)
        coef = jnp.where(sub == 1 + c, rate, coef)
    coef_ref[...] = coef
    for item in column_copies:
        item.wait_send()


def update_kernel(force_in, coef_ref, pos_ref, vel_ref, par_ref, force_ref, nvel_ref, npos_ref, coup_ref):
    coef = coef_ref[...]
    for k in range(4):
        coup_ref[k] = coef[k, 0]
    drag, grow = coef[0:1] + coef[1:4], 1.0 + time_step * coef[1:4]
    for t in range(pos_ref.shape[1] // L):
        cols = slice(t * L, (t + 1) * L)
        f, v = force_in[:, cols], vel_ref[:, cols]
        v = v + time_step * (f * par_ref[3:4, cols] - drag * v)
        force_ref[:, cols] = f
        nvel_ref[:, cols] = v
        npos_ref[:, cols] = pos_ref[:, cols] * grow + time_step * v


def on_device(
    positions,
    velocities,
    atom_params,
    pair_list,
    pair_count,
    exclusion,
    halo_far,
    box_lengths,
    extended_variables,
):
    domains = lax.axis_size("gx")
    planes = domains // PLANE
    atoms, fars = positions.shape[1], halo_far.shape[0]
    clusters, groups = atoms // 8, WIDTH // L
    vmem = pl.BlockSpec(memory_space=pltpu.VMEM)
    rows = jax.ShapeDtypeStruct((3, atoms), F32)
    dma = pltpu.SemaphoreType.DMA
    forces, coef = pl.pallas_call(
        functools.partial(step_kernel, domains),
        out_shape=(rows, jax.ShapeDtypeStruct((8, L), F32)),
        in_specs=[pl.BlockSpec(memory_space=pltpu.HBM)] * 9,
        out_specs=(vmem, vmem),
        scratch_shapes=[
            pltpu.SMEM((1,), I32),
            pltpu.SMEM((3,), F32),
            pltpu.SMEM((4,), F32),
            pltpu.VMEM((1, fars), I32),
            pltpu.VMEM((3, atoms), F32),
            pltpu.VMEM((3, atoms), F32),
            pltpu.VMEM((4, atoms), F32),
            pltpu.VMEM(pair_list.shape, I32),
            pltpu.VMEM(exclusion.shape, I32),
            pltpu.VMEM((3, atoms), F32),
            pltpu.VMEM((4, atoms), F32),
            pltpu.VMEM((6, 8, L), F32),
            pltpu.VMEM((6, 8, L), F32),
            pltpu.VMEM((2, 24, L), F32),
            pltpu.VMEM((24, L), F32),
            pltpu.VMEM((2, 24, L), F32),
            pltpu.VMEM((24, L), F32),
            pltpu.VMEM((8, L), F32),
            pltpu.VMEM((1, L), F32),
            pltpu.VMEM((1, L), F32),
            pltpu.VMEM((PLANE, 1, L), F32),
            pltpu.VMEM((planes, 1, L), F32),
            pltpu.VMEM((6, 8, 2 * L), F32),
            pltpu.VMEM((6, 8, 4 * L), F32),
            pltpu.VMEM((groups, 6, 16, L), F32),
            pltpu.VMEM((groups, 6, 8, L), F32),
            pltpu.VMEM((groups, 8, L), I32),
            pltpu.VMEM((groups, 6, 8, L), F32),
            pltpu.VMEM((192, L), F32),
            pltpu.VMEM((96, clusters // 2), F32),
            pltpu.VMEM((3, 8, L), F32),
            dma((9,)),
            dma((3,)),
            dma((3,)),
            dma((2,)),
            dma((2,)),
            dma((PLANE - 1,)),
            dma((PLANE,)),
            dma((planes - 1,)),
            dma((planes,)),
            pltpu.SemaphoreType.REGULAR((2 * planes.bit_length(),)),
        ],
        compiler_params=pltpu.CompilerParams(collective_id=0, has_side_effects=True),
        name="force_step",
    )(pair_count, box_lengths, extended_variables, halo_far[None], positions, velocities, atom_params,
      pair_list, exclusion)
    return pl.pallas_call(
        update_kernel,
        out_shape=(rows, rows, rows, jax.ShapeDtypeStruct((4,), F32)),
        in_specs=[vmem] * 5,
        out_specs=(vmem, vmem, vmem, pl.BlockSpec(memory_space=pltpu.SMEM)),
        name="update",
    )(forces, coef, positions, velocities, atom_params)


def solution(mesh):
    whole = ("rep", "gx")
    rows, flat = P(None, whole), P(whole)
    return jax.shard_map(
        on_device,
        mesh=mesh,
        in_specs=(rows, rows, rows, rows, flat, rows, flat, P("rep"), P("rep")),
        out_specs=(rows, rows, rows, P("rep")),
        check_vma=False,
    )
```

```python
import functools

import jax
import jax.numpy as jnp
from jax import lax
from jax.experimental import pallas as pl
from jax.experimental.pallas import tpu as pltpu
from jax.sharding import PartitionSpec as P

PLANE = 8
WIDTH = 512
MESH = pl.DeviceIdType.MESH

time_step = 0.25
thermal_scale_unit = 2.0
reservoir_inertia_mass = 4.0
barostat_gain = 0.1
pressure_target = 1.0

RT = 1.0 / 1331.0
L = 128
F32, BF16, I16, I32 = jnp.float32, jnp.bfloat16, jnp.int16, jnp.int32


def take(x, idx):
    dn = lax.GatherDimensionNumbers(offset_dims=(), collapsed_slice_dims=(1,), start_index_map=(1,),
                                    operand_batching_dims=(0,), start_indices_batching_dims=(0,))
    return lax.gather(x, idx[:, :, None], dn, (1, 1), mode=lax.GatherScatterMode.PROMISE_IN_BOUNDS)


def iota(shape, dim):
    return lax.broadcasted_iota(I32, shape, dim)


def to_cluster_rows(row, clusters):
    lane, sub = iota((8, L), 1), iota((8, L), 0)
    idx = 8 * (lane % 16) + sub
    part = lane // 16
    tiles = []
    for t in range((clusters + L - 1) // L):
        out = None
        for u in range(8):
            start = (8 * t + u) * L
            if start >= 8 * clusters:
                break
            got = take(row(start), idx)
            out = got if out is None else jnp.where(part == u, got, out)
        tiles.append(out)
    return tiles


def step_kernel(
    domains, count_in, box_in, ext_in, halo_in, pos_in, vel_in, par_in, pl_in, ex_in,
    force_ref, coef_ref,
    count_ref, box_ref, ext_ref, halo_ref, pos_ref, vel_ref, par_ref, pl_ref, ex_ref,
    near_out, mix_out, far_out, mix_in, near_force, far_force, near_in, far_in,
    part, src1, src2, sum1, sum2,
    tab_i, tab_j, jd, ri, wd, fs, acc_j, acc_i, vacc,
    load_sem, halo_send, halo_recv, force_send, force_recv, send1, recv1, send2, recv2, relay,
):
    planes = domains // PLANE
    me = lax.axis_index("gx")
    place, plane = lax.rem(me, PLANE), lax.div(me, PLANE)
    at = lambda shift: lax.rem(me + domains + shift, domains)
    column = lambda shift: lax.rem(plane + planes + shift, planes) * PLANE + place
    mates = [plane * PLANE + lax.rem(place + k, PLANE) for k in range(1, PLANE)]
    steps = sorted(range(1, planes), key=lambda k: min(k, planes - k))
    columns = [column(k) for k in steps]

    barrier = pltpu.get_barrier_semaphore()
    greeted = [at(2), at(1), at(-1), at(-2), column(1), column(-1)] + mates
    for other in greeted:
        pl.semaphore_signal(barrier, inc=1, device_id={"gx": other}, device_id_type=MESH)

    loads = [
        pltpu.make_async_copy(src, dst, load_sem.at[k])
        for k, (src, dst) in enumerate((
            (pos_in, pos_ref), (par_in, par_ref), (halo_in, halo_ref), (box_in, box_ref), (vel_in, vel_ref),
            (count_in, count_ref), (ext_in, ext_ref), (pl_in, pl_ref), (ex_in, ex_ref),
        ))
    ]
    for item in loads:
        item.start()

    def copy(src, dst, send, recv, other):
        return pltpu.make_async_remote_copy(
            src_ref=src, dst_ref=dst, send_sem=send, recv_sem=recv, device_id={"gx": other}, device_id_type=MESH
        )

    halo_copies = [
        copy(near_out, tab_j.at[2], halo_send.at[0], halo_recv.at[0], at(-1)),
        copy(mix_out, mix_in, halo_send.at[1], halo_recv.at[1], at(-1)),
        copy(far_out, tab_j.at[3], halo_send.at[2], halo_recv.at[2], at(-2)),
    ]
    for item in loads[:4]:
        item.wait()

    clusters = pos_ref.shape[1] // 8
    fars = halo_ref.shape[1]
    width = fs.shape[0] * L
    box = [box_ref[c] for c in range(3)]

    def row_of(c):
        def row(start):
            ref, r = (pos_ref, c) if c < 3 else (par_ref, c - 3)
            return jnp.broadcast_to(ref[pl.ds(r, 1), pl.ds(start, L)], (8, L))
        return row

    lane8 = iota((8, L), 1)
    tiles_of = clusters // 16
    half = clusters - L
    scales = (1.0, 1.0, 1.0, 1.0, 6.0, 12.0)
    hal = jnp.concatenate(
        [jnp.broadcast_to(halo_ref[...], (8, fars)), jnp.zeros((8, L - fars), I32)], axis=1)
    lifts = [jnp.where(me < k, box[0], 0.0) for k in (1, 2)]
    heads = []
    for c in range(6):
        own = to_cluster_rows(row_of(c), clusters)
        for t in range(2):
            tab_i[c, :, t * L:(t + 1) * L] = own[t] * scales[c] if scales[c] != 1.0 else own[t]
            tab_j[t, c] = own[t]
        far = jnp.where(hal >= L, take(own[1], hal & (L - 1)), take(own[0], hal & (L - 1)))
        far_out[c] = far + lifts[1] if c == 0 else far
        if c == 0:
            own = [v + lifts[0] for v in own]
        rot0, rot1 = pltpu.roll(own[0], half, 1), pltpu.roll(own[1], half, 1)
        near_out[c] = jnp.where(lane8 < half, rot0, rot1)
        if c < 3:
            heads.append(rot0)
        else:
            mix_out[c - 3] = jnp.where(lane8 < half, own[0], heads[c - 3])
    pl.semaphore_wait(barrier, len(greeted))
    for item in halo_copies:
        item.start()

    def tell(round_, distance):
        for side in (0, 1):
            pl.semaphore_signal(
                relay.at[2 * round_ + side], inc=1,
                device_id={"gx": column(distance if side else -distance)}, device_id_type=MESH)

    def hear(round_):
        for side in (0, 1):
            pl.semaphore_wait(relay.at[2 * round_ + side], 1)

    distances = []
    while 2 ** (len(distances) + 1) < planes:
        distances.append(2 ** len(distances))
    tell(0, distances[0])

    for item in loads[4:]:
        item.wait()
    part[...] = jnp.zeros_like(part)
    kin = None
    for t in range(tiles_of):
        cols = slice(t * L, (t + 1) * L)
        term = vel_ref[:, cols] * vel_ref[:, cols] / par_ref[3:4, cols]
        kin = term if kin is None else kin + term
    part[0:3, :] = 0.5 * kin
    acc_j[...] = jnp.zeros_like(acc_j)
    acc_i[...] = jnp.zeros_like(acc_i)
    vacc[...] = jnp.zeros_like(vacc)
    fs[...] = jnp.zeros_like(fs)

    for item in halo_copies:
        item.wait()
    for c in range(3):
        mixed = mix_in[c]
        tab_j[1, c] = jnp.where(lane8 < half, tab_j[1, c], mixed)
        tab_j[1, c + 3] = jnp.where(lane8 < half, tab_j[1, c + 3], pltpu.roll(mixed, half, 1))

    sub = iota((8, L), 0)
    count = count_ref[0]
    shift0 = 8 * (sub % 2)
    bits = [jnp.left_shift(1, shift0 + ((sub + m) & 7)) for m in range(8)]
    one16 = jnp.ones((16, L), BF16)
    zero16 = jnp.zeros((16, L), BF16)

    groups = width // L
    bases = [(iota((16, L), 0) + 16 * r).astype(I16) for r in range(L // 16)]

    def gather(block):
        for g in range(groups):
            first = block * width + g * L
            cols = pl.ds(pl.multiple_of(first, L), L)
            ib = jnp.broadcast_to(pl_ref[pl.ds(0, 1), cols], (8, L))
            jb = jnp.broadcast_to(pl_ref[pl.ds(1, 1), cols], (8, L))
            sb = jnp.broadcast_to(pl_ref[pl.ds(2, 1), cols], (8, L))
            usable = lane8 < count - first
            w = [jnp.broadcast_to(ex_ref[pl.ds(k, 1), cols], (8, L)) for k in range(4)]
            words = jnp.where(sub < 4, jnp.where(sub < 2, w[0], w[1]), jnp.where(sub < 6, w[2], w[3]))
            wd[g] = jnp.where(usable, words, 0)
            above_y, below_y = sb >= 6, sb < 3
            s3 = sb - jnp.where(above_y, 6, jnp.where(below_y, 0, 3))
            il, ih = ib & (L - 1), ib >= L
            jl, jh, jm = jb & (L - 1), jb >= 2 * L, (jb & L) != 0
            for c in range(6):
                v = jnp.where(ih, take(tab_i[c, :, L:2 * L], il), take(tab_i[c, :, 0:L], il))
                if c in (1, 2):
                    v = v - jnp.where(above_y if c == 1 else s3 == 2, box[c], 0.0)
                ri[g, c] = v
            for c in range(6):
                q = [take(tab_j[t, c], jl) for t in range(4)]
                v = jnp.where(jh, jnp.where(jm, q[3], q[2]), jnp.where(jm, q[1], q[0]))
                if c in (1, 2):
                    v = v - jnp.where(below_y if c == 1 else s3 == 0, box[c], 0.0)
                jd[g, c, 0:8, :] = v
                jd[g, c, 8:16, :] = v

    def split(fs):
        hi = [f.astype(BF16).astype(F32) for f in fs]
        lo = [f - h for f, h in zip(fs, hi)]
        return jnp.concatenate(hi + lo, axis=0).astype(BF16)

    def compute(block):
        for g in range(groups):
            xi, yi, zi, qi, ei, bi = [ri[g, c] for c in range(6)]
            words = wd[g]
            fi, fj = [None] * 3, [None] * 3
            for m in range(7, -1, -1):
                xj, yj, zj, qj, ej, bj = [jd[g, c, m:m + 8, :] for c in range(6)]
                d = (xj - xi, yj - yi, zj - zi)
                r2 = d[0] * d[0] + d[1] * d[1] + d[2] * d[2]
                inv = lax.rsqrt(r2)
                inv2 = inv * inv
                inv3 = inv * inv2
                inv6 = inv3 * inv3
                s = qi * qj * (inv3 - RT) + (bi * bj * inv6 - ei * ej) * (inv6 * inv2)
                s = jnp.where((words & bits[m]) != 0, s, 0.0)
                for c in range(3):
                    f = s * d[c]
                    fi[c] = f if fi[c] is None else fi[c] + f
                    fj[c] = f if fj[c] is None else pltpu.roll(fj[c], 1, 0) + f
            for c, v in enumerate((xi, yi, zi)):
                origin = jnp.broadcast_to(ri[g, c, 0:1, :], (8, L))
                vacc[c] += fj[c] * (jd[g, c, 0:8, :] - origin) - fi[c] * (v - origin)
            for c in range(3):
                fs[g, c] = fj[c]
                fs[g, 3 + c] = fi[c]

    half_c = clusters // 2

    def dots(block):
        tjs, tis, ojs, ois = [], [], [], []
        for g in range(groups):
            cols = pl.ds(pl.multiple_of(block * width + g * L, L), L)
            j16 = jnp.broadcast_to(pl_ref[pl.ds(1, 1), cols], (16, L)).astype(I16)
            i16 = jnp.broadcast_to(pl_ref[pl.ds(0, 1), cols], (16, L)).astype(I16)
            tj = split([fs[g, c] for c in range(3)])
            ti = split([fs[g, 3 + c] for c in range(3)])
            parts = lambda t: [t[16 * r:16 * r + 16] for r in range(3)]
            which = j16 & (3 * L)
            tjs.append(jnp.concatenate(
                [jnp.where(which == k * L, p, zero16) for k in range(4) for p in parts(tj)], axis=0))
            later = i16 >= half_c
            tis.append(jnp.concatenate(
                [jnp.where(later, zero16, p) for p in parts(ti)] + [jnp.where(later, p, zero16) for p in parts(ti)], axis=0))
            j16 = j16 & (L - 1)
            i16 = jnp.where(later, i16 - half_c, i16)
            ojs.append(jnp.concatenate([jnp.where(bases[r] == j16, one16, zero16) for r in range(L // 16)], axis=0))
            ois.append(jnp.concatenate([jnp.where(bases[r] == i16, one16, zero16) for r in range(half_c // 16)], axis=0))
        contract = (((1,), (1,)), ((), ()))
        wide = lambda xs: jnp.concatenate(xs, axis=1)
        acc_j[...] += lax.dot_general(wide(tjs), wide(ojs), contract, preferred_element_type=F32)
        acc_i[...] += lax.dot_general(wide(tis), wide(ois), contract, preferred_element_type=F32)

    blocks = pl_ref.shape[1] // width

    def step(block, carry):
        dots(jnp.maximum(block - 1, 0))
        compute(block)
        gather(jnp.minimum(block + 1, blocks - 1))
        return carry

    gather(0)
    rounds = len(distances)
    marks = [0] + [5 + 7 * k for k in range(rounds - 1)] + [blocks]
    for k in range(rounds):
        lax.fori_loop(marks[k], marks[k + 1], step, 0)
        if k + 1 < rounds:
            hear(k)
            tell(k + 1, distances[k + 1])
    for c in range(3):
        part[3 + c:4 + c, :] = -0.5 * jnp.sum(vacc[c], axis=0, keepdims=True)
    sums = jnp.sum(part[...], axis=1, keepdims=True)
    row = jnp.sum(jnp.where(sub == lane8, jnp.broadcast_to(sums, (8, L)), 0.0), axis=0, keepdims=True)
    src1[...] = row
    sum1[place] = src1[...]
    plane_copies = [
        copy(src1, sum1.at[place], send1.at[k], recv1.at[place], mate) for k, mate in enumerate(mates)]
    for item in plane_copies:
        item.start()
    dots(blocks - 1)
    tile_at = lambda k: acc_j[48 * k:48 * k + 24] + acc_j[48 * k + 24:48 * k + 48]
    near_force[0] = tile_at(1)
    near_force[1] = tile_at(2)
    far_force[...] = tile_at(3)
    near_copy = copy(near_force, near_in, force_send.at[0], force_recv.at[0], at(1))
    far_copy = copy(far_force, far_in, force_send.at[1], force_recv.at[1], at(2))
    far_copy.start()
    near_copy.start()
    tiles = [tile_at(0), near_force[0]]
    pad = jnp.zeros((24, L - half_c), F32)
    mi = [acc_i[48 * k:48 * k + 24] + acc_i[48 * k + 24:48 * k + 48] for k in range(2)]
    mi = [jnp.concatenate([v, pad], axis=1) for v in mi]
    hal1 = jnp.concatenate([halo_ref[...], jnp.full((1, L - fars), 4 * L, I32)], axis=1)
    oh_far = (jnp.broadcast_to(hal1, (clusters, L)) == iota((clusters, L), 0)).astype(F32).astype(BF16)

    hear(rounds - 1)
    for k in range(1, PLANE):
        other = lax.rem(place + k, PLANE)
        copy(src1, sum1.at[other], send1.at[k - 1], recv1.at[other], mates[k - 1]).wait_recv()
    row = sum1[0]
    for k in range(1, PLANE):
        row = row + sum1[k]
    src2[...] = row
    sum2[plane] = src2[...]
    column_copies = [
        copy(src2, sum2.at[plane], send2.at[k], recv2.at[plane], other) for k, other in enumerate(columns)]
    for item in column_copies:
        item.start()

    near_copy.wait()
    far_copy.wait()
    ff = far_in[...]
    f1 = ff.astype(BF16)
    r1 = ff - f1.astype(F32)
    f2 = r1.astype(BF16)
    f3 = (r1 - f2.astype(F32)).astype(BF16)
    far = sum(lax.dot_general(f, oh_far, (((1,), (1,)), ((), ())), preferred_element_type=F32) for f in (f3, f2, f1))
    tiles[0] = tiles[0] + far[:, 0:L]
    tiles[1] = tiles[1] + jnp.concatenate([far[:, L:], jnp.zeros((24, 2 * L - clusters), F32)], axis=1)
    back = [near_in[0], near_in[1]]
    pick = sub == (lane8 & 7)
    for c in range(3):
        for t in range(tiles_of):
            def window(tabs, slot, size):
                return take(tabs[slot // size][8 * c:8 * c + 8], slot % size + lane8 // 8)
            got = window(tiles, 16 * t, L) - window(mi, 16 * t, half_c) + window(back, half + 16 * t, L)
            force_ref[c:c + 1, t * L:(t + 1) * L] = jnp.sum(jnp.where(pick, got, 0.0), axis=0, keepdims=True)

    for item in plane_copies:
        item.wait_send()
    for k, step_ in enumerate(steps):
        other = lax.rem(plane + step_, planes)
        copy(src2, sum2.at[other], send2.at[k], recv2.at[other], columns[k]).wait_recv()
    row = sum2[0]
    for k in range(1, planes):
        row = row + sum2[k]
    row = jnp.broadcast_to(row, (8, L))
    one_of = [take(row, jnp.full((8, L), c, I32)) for c in range(6)]
    total = one_of[0] + one_of[1] + one_of[2]
    volume = box[0] * box[1] * box[2]
    ratio = 2.0 * total / (3.0 * (8 * clusters * domains) * thermal_scale_unit)
    coef = ext_ref[0] + reservoir_inertia_mass * (ratio - 1.0)
    for c in range(3):
        rate = ext_ref[1 + c] + barostat_gain * (
            one_of[c] - one_of[3 + c] - pressure_target * volume / 2.0
        ) / (total / 3.0)
        coef = jnp.where(sub == 1 + c, rate, coef)
    coef_ref[...] = coef
    for item in column_copies:
        item.wait_send()


def update_kernel(force_in, coef_ref, pos_ref, vel_ref, par_ref, force_ref, nvel_ref, npos_ref, coup_ref):
    coef = coef_ref[...]
    for k in range(4):
        coup_ref[k] = coef[k, 0]
    drag, grow = coef[0:1] + coef[1:4], 1.0 + time_step * coef[1:4]
    for t in range(pos_ref.shape[1] // L):
        cols = slice(t * L, (t + 1) * L)
        f, v = force_in[:, cols], vel_ref[:, cols]
        v = v + time_step * (f * par_ref[3:4, cols] - drag * v)
        force_ref[:, cols] = f
        nvel_ref[:, cols] = v
        npos_ref[:, cols] = pos_ref[:, cols] * grow + time_step * v


def on_device(
    positions,
    velocities,
    atom_params,
    pair_list,
    pair_count,
    exclusion,
    halo_far,
    box_lengths,
    extended_variables,
):
    domains = lax.axis_size("gx")
    planes = domains // PLANE
    atoms, fars = positions.shape[1], halo_far.shape[0]
    clusters, groups = atoms // 8, WIDTH // L
    vmem = pl.BlockSpec(memory_space=pltpu.VMEM)
    rows = jax.ShapeDtypeStruct((3, atoms), F32)
    dma = pltpu.SemaphoreType.DMA
    forces, coef = pl.pallas_call(
        functools.partial(step_kernel, domains),
        out_shape=(rows, jax.ShapeDtypeStruct((8, L), F32)),
        in_specs=[pl.BlockSpec(memory_space=pltpu.HBM)] * 9,
        out_specs=(vmem, vmem),
        scratch_shapes=[
            pltpu.SMEM((1,), I32),
            pltpu.SMEM((3,), F32),
            pltpu.SMEM((4,), F32),
            pltpu.VMEM((1, fars), I32),
            pltpu.VMEM((3, atoms), F32),
            pltpu.VMEM((3, atoms), F32),
            pltpu.VMEM((4, atoms), F32),
            pltpu.VMEM(pair_list.shape, I32),
            pltpu.VMEM(exclusion.shape, I32),
            pltpu.VMEM((6, 8, L), F32),
            pltpu.VMEM((3, 8, L), F32),
            pltpu.VMEM((6, 8, L), F32),
            pltpu.VMEM((3, 8, L), F32),
            pltpu.VMEM((2, 24, L), F32),
            pltpu.VMEM((24, L), F32),
            pltpu.VMEM((2, 24, L), F32),
            pltpu.VMEM((24, L), F32),
            pltpu.VMEM((8, L), F32),
            pltpu.VMEM((1, L), F32),
            pltpu.VMEM((1, L), F32),
            pltpu.VMEM((PLANE, 1, L), F32),
            pltpu.VMEM((planes, 1, L), F32),
            pltpu.VMEM((6, 8, 2 * L), F32),
            pltpu.VMEM((4, 6, 8, L), F32),
            pltpu.VMEM((groups, 6, 16, L), F32),
            pltpu.VMEM((groups, 6, 8, L), F32),
            pltpu.VMEM((groups, 8, L), I32),
            pltpu.VMEM((groups, 6, 8, L), F32),
            pltpu.VMEM((192, L), F32),
            pltpu.VMEM((96, clusters // 2), F32),
            pltpu.VMEM((3, 8, L), F32),
            dma((9,)),
            dma((3,)),
            dma((3,)),
            dma((2,)),
            dma((2,)),
            dma((PLANE - 1,)),
            dma((PLANE,)),
            dma((planes - 1,)),
            dma((planes,)),
            pltpu.SemaphoreType.REGULAR((2 * planes.bit_length(),)),
        ],
        compiler_params=pltpu.CompilerParams(
            collective_id=0, has_side_effects=True, vmem_limit_bytes=50000 * 1024),
        name="force_step",
    )(pair_count, *[pltpu.with_memory_space_constraint(x, pltpu.HBM) for x in (box_lengths, extended_variables, halo_far[None], positions, velocities, atom_params,
      pair_list, exclusion)])
    return pl.pallas_call(
        update_kernel,
        out_shape=(rows, rows, rows, jax.ShapeDtypeStruct((4,), F32)),
        in_specs=[vmem] * 5,
        out_specs=(vmem, vmem, vmem, pl.BlockSpec(memory_space=pltpu.SMEM)),
        compiler_params=pltpu.CompilerParams(vmem_limit_bytes=8000 * 1024),
        name="update",
    )(forces, coef, positions, velocities, atom_params)


def solution(mesh):
    whole = ("rep", "gx")
    rows, flat = P(None, whole), P(whole)
    return jax.shard_map(
        on_device,
        mesh=mesh,
        in_specs=(rows, rows, rows, rows, flat, rows, flat, P("rep"), P("rep")),
        out_specs=(rows, rows, rows, P("rep")),
        check_vma=False,
    )
```

```python
import functools

import jax
import jax.numpy as jnp
from jax import lax
from jax.experimental import pallas as pl
from jax.experimental.pallas import tpu as pltpu
from jax.sharding import PartitionSpec as P

PLANE = 8
WIDTH = 512
MESH = pl.DeviceIdType.MESH

time_step = 0.25
thermal_scale_unit = 2.0
reservoir_inertia_mass = 4.0
barostat_gain = 0.1
pressure_target = 1.0

RT = 1.0 / 1331.0
L = 128
F32, BF16, I16, I32 = jnp.float32, jnp.bfloat16, jnp.int16, jnp.int32


def take(x, idx):
    dn = lax.GatherDimensionNumbers(offset_dims=(), collapsed_slice_dims=(1,), start_index_map=(1,),
                                    operand_batching_dims=(0,), start_indices_batching_dims=(0,))
    return lax.gather(x, idx[:, :, None], dn, (1, 1), mode=lax.GatherScatterMode.PROMISE_IN_BOUNDS)


def iota(shape, dim):
    return lax.broadcasted_iota(I32, shape, dim)


def to_cluster_rows(row, clusters):
    lane, sub = iota((8, L), 1), iota((8, L), 0)
    idx = 8 * (lane % 16) + sub
    part = lane // 16
    tiles = []
    for t in range((clusters + L - 1) // L):
        out = None
        for u in range(8):
            start = (8 * t + u) * L
            if start >= 8 * clusters:
                break
            got = take(row(start), idx)
            out = got if out is None else jnp.where(part == u, got, out)
        tiles.append(out)
    return tiles


def step_kernel(
    domains, count_in, box_in, ext_in, halo_in, pos_in, vel_in, par_in, pl_in, ex_in,
    force_ref, coef_ref,
    count_ref, box_ref, ext_ref, halo_ref, pos_ref, vel_ref, par_ref, pl_ref, ex_ref,
    near_out, mix_out, far_out, mix_in, near_force, far_force, near_in, far_in,
    part, src1, src2, sum1, prev1, sum2,
    tab_i, tab_j, jd, ri, wd, fs, acc_j, acc_i, vacc,
    load_sem, halo_send, halo_recv, force_send, force_recv, send1, recv1, send3, recv3, send2, recv2, relay,
):
    planes = domains // PLANE
    me = lax.axis_index("gx")
    place, plane = lax.rem(me, PLANE), lax.div(me, PLANE)
    at = lambda shift: lax.rem(me + domains + shift, domains)
    column = lambda shift: lax.rem(plane + planes + shift, planes) * PLANE + place
    mates = [plane * PLANE + lax.rem(place + k, PLANE) for k in range(1, PLANE)]
    steps = sorted(range(2, planes), key=lambda k: min(k, planes - k))
    columns = [column(k) for k in steps]

    barrier = pltpu.get_barrier_semaphore()
    greeted = [at(2), at(1), at(-1), at(-2), column(1), column(-1)] + mates
    for other in greeted:
        pl.semaphore_signal(barrier, inc=1, device_id={"gx": other}, device_id_type=MESH)

    loads = [
        pltpu.make_async_copy(src, dst, load_sem.at[k])
        for k, (src, dst) in enumerate((
            (pos_in, pos_ref), (par_in, par_ref), (halo_in, halo_ref), (box_in, box_ref), (vel_in, vel_ref),
            (count_in, count_ref), (ext_in, ext_ref), (pl_in, pl_ref), (ex_in, ex_ref),
        ))
    ]
    for item in loads:
        item.start()

    def copy(src, dst, send, recv, other):
        return pltpu.make_async_remote_copy(
            src_ref=src, dst_ref=dst, send_sem=send, recv_sem=recv, device_id={"gx": other}, device_id_type=MESH
        )

    halo_copies = [
        copy(near_out, tab_j.at[2], halo_send.at[0], halo_recv.at[0], at(-1)),
        copy(mix_out, mix_in, halo_send.at[1], halo_recv.at[1], at(-1)),
        copy(far_out, tab_j.at[3], halo_send.at[2], halo_recv.at[2], at(-2)),
    ]
    for item in loads[:4]:
        item.wait()

    clusters = pos_ref.shape[1] // 8
    fars = halo_ref.shape[1]
    width = fs.shape[0] * L
    box = [box_ref[c] for c in range(3)]

    def row_of(c):
        def row(start):
            ref, r = (pos_ref, c) if c < 3 else (par_ref, c - 3)
            return jnp.broadcast_to(ref[pl.ds(r, 1), pl.ds(start, L)], (8, L))
        return row

    lane8 = iota((8, L), 1)
    tiles_of = clusters // 16
    half = clusters - L
    scales = (1.0, 1.0, 1.0, 1.0, 6.0, 12.0)
    hal = jnp.concatenate(
        [jnp.broadcast_to(halo_ref[...], (8, fars)), jnp.zeros((8, L - fars), I32)], axis=1)
    lifts = [jnp.where(me < k, box[0], 0.0) for k in (1, 2)]
    heads = []
    for c in range(6):
        own = to_cluster_rows(row_of(c), clusters)
        for t in range(2):
            tab_i[c, :, t * L:(t + 1) * L] = own[t] * scales[c] if scales[c] != 1.0 else own[t]
            tab_j[t, c] = own[t]
        far = jnp.where(hal >= L, take(own[1], hal & (L - 1)), take(own[0], hal & (L - 1)))
        far_out[c] = far + lifts[1] if c == 0 else far
        if c == 0:
            own = [v + lifts[0] for v in own]
        rot0, rot1 = pltpu.roll(own[0], half, 1), pltpu.roll(own[1], half, 1)
        near_out[c] = jnp.where(lane8 < half, rot0, rot1)
        if c < 3:
            heads.append(rot0)
        else:
            mix_out[c - 3] = jnp.where(lane8 < half, own[0], heads[c - 3])
    pl.semaphore_wait(barrier, len(greeted))
    for item in halo_copies:
        item.start()

    def tell(round_, distance):
        for side in (0, 1):
            pl.semaphore_signal(
                relay.at[2 * round_ + side], inc=1,
                device_id={"gx": column(distance if side else -distance)}, device_id_type=MESH)

    def hear(round_):
        for side in (0, 1):
            pl.semaphore_wait(relay.at[2 * round_ + side], 1)

    distances = []
    while 2 ** (len(distances) + 1) < planes:
        distances.append(2 ** len(distances))
    tell(0, distances[0])

    for item in loads[4:]:
        item.wait()
    part[...] = jnp.zeros_like(part)
    kin = None
    for t in range(tiles_of):
        cols = slice(t * L, (t + 1) * L)
        term = vel_ref[:, cols] * vel_ref[:, cols] / par_ref[3:4, cols]
        kin = term if kin is None else kin + term
    part[0:3, :] = 0.5 * kin
    acc_j[...] = jnp.zeros_like(acc_j)
    acc_i[...] = jnp.zeros_like(acc_i)
    vacc[...] = jnp.zeros_like(vacc)
    fs[...] = jnp.zeros_like(fs)

    for item in halo_copies:
        item.wait()
    for c in range(3):
        mixed = mix_in[c]
        tab_j[1, c] = jnp.where(lane8 < half, tab_j[1, c], mixed)
        tab_j[1, c + 3] = jnp.where(lane8 < half, tab_j[1, c + 3], pltpu.roll(mixed, half, 1))

    sub = iota((8, L), 0)
    count = count_ref[0]
    shift0 = 8 * (sub % 2)
    bits = [jnp.left_shift(1, shift0 + ((sub + m) & 7)) for m in range(8)]
    one16 = jnp.ones((16, L), BF16)
    zero16 = jnp.zeros((16, L), BF16)

    groups = width // L
    bases = [(iota((16, L), 0) + 16 * r).astype(I16) for r in range(L // 16)]

    def gather(block):
        for g in range(groups):
            first = block * width + g * L
            cols = pl.ds(pl.multiple_of(first, L), L)
            ib = jnp.broadcast_to(pl_ref[pl.ds(0, 1), cols], (8, L))
            jb = jnp.broadcast_to(pl_ref[pl.ds(1, 1), cols], (8, L))
            sb = jnp.broadcast_to(pl_ref[pl.ds(2, 1), cols], (8, L))
            usable = lane8 < count - first
            w = [jnp.broadcast_to(ex_ref[pl.ds(k, 1), cols], (8, L)) for k in range(4)]
            words = jnp.where(sub < 4, jnp.where(sub < 2, w[0], w[1]), jnp.where(sub < 6, w[2], w[3]))
            wd[g] = jnp.where(usable, words, 0)
            above_y, below_y = sb >= 6, sb < 3
            s3 = sb - jnp.where(above_y, 6, jnp.where(below_y, 0, 3))
            il, ih = ib & (L - 1), ib >= L
            jl, jh, jm = jb & (L - 1), jb >= 2 * L, (jb & L) != 0
            for c in range(6):
                v = jnp.where(ih, take(tab_i[c, :, L:2 * L], il), take(tab_i[c, :, 0:L], il))
                if c in (1, 2):
                    v = v - jnp.where(above_y if c == 1 else s3 == 2, box[c], 0.0)
                ri[g, c] = v
            for c in range(6):
                q = [take(tab_j[t, c], jl) for t in range(4)]
                v = jnp.where(jh, jnp.where(jm, q[3], q[2]), jnp.where(jm, q[1], q[0]))
                if c in (1, 2):
                    v = v - jnp.where(below_y if c == 1 else s3 == 0, box[c], 0.0)
                jd[g, c, 0:8, :] = v
                jd[g, c, 8:16, :] = v

    def split(fs):
        hi = [f.astype(BF16).astype(F32) for f in fs]
        lo = [f - h for f, h in zip(fs, hi)]
        return jnp.concatenate(hi + lo, axis=0).astype(BF16)

    def compute(block):
        for g in range(groups):
            xi, yi, zi, qi, ei, bi = [ri[g, c] for c in range(6)]
            words = wd[g]
            fi, fj = [None] * 3, [None] * 3
            for m in range(7, -1, -1):
                xj, yj, zj, qj, ej, bj = [jd[g, c, m:m + 8, :] for c in range(6)]
                d = (xj - xi, yj - yi, zj - zi)
                r2 = d[0] * d[0] + d[1] * d[1] + d[2] * d[2]
                inv = lax.rsqrt(r2)
                inv2 = inv * inv
                inv3 = inv * inv2
                inv6 = inv3 * inv3
                s = qi * qj * (inv3 - RT) + (bi * bj * inv6 - ei * ej) * (inv6 * inv2)
                s = jnp.where((words & bits[m]) != 0, s, 0.0)
                for c in range(3):
                    f = s * d[c]
                    fi[c] = f if fi[c] is None else fi[c] + f
                    fj[c] = f if fj[c] is None else pltpu.roll(fj[c], 1, 0) + f
            for c, v in enumerate((xi, yi, zi)):
                origin = jnp.broadcast_to(ri[g, c, 0:1, :], (8, L))
                vacc[c] += fj[c] * (jd[g, c, 0:8, :] - origin) - fi[c] * (v - origin)
            for c in range(3):
                fs[g, c] = fj[c]
                fs[g, 3 + c] = fi[c]

    half_c = clusters // 2

    def dots(block):
        tjs, tis, ojs, ois = [], [], [], []
        for g in range(groups):
            cols = pl.ds(pl.multiple_of(block * width + g * L, L), L)
            j16 = jnp.broadcast_to(pl_ref[pl.ds(1, 1), cols], (16, L)).astype(I16)
            i16 = jnp.broadcast_to(pl_ref[pl.ds(0, 1), cols], (16, L)).astype(I16)
            tj = split([fs[g, c] for c in range(3)])
            ti = split([fs[g, 3 + c] for c in range(3)])
            parts = lambda t: [t[16 * r:16 * r + 16] for r in range(3)]
            which = j16 & (3 * L)
            tjs.append(jnp.concatenate(
                [jnp.where(which == k * L, p, zero16) for k in range(4) for p in parts(tj)], axis=0))
            later = i16 >= half_c
            tis.append(jnp.concatenate(
                [jnp.where(later, zero16, p) for p in parts(ti)] + [jnp.where(later, p, zero16) for p in parts(ti)], axis=0))
            j16 = j16 & (L - 1)
            i16 = jnp.where(later, i16 - half_c, i16)
            ojs.append(jnp.concatenate([jnp.where(bases[r] == j16, one16, zero16) for r in range(L // 16)], axis=0))
            ois.append(jnp.concatenate([jnp.where(bases[r] == i16, one16, zero16) for r in range(half_c // 16)], axis=0))
        contract = (((1,), (1,)), ((), ()))
        wide = lambda xs: jnp.concatenate(xs, axis=1)
        acc_j[...] += lax.dot_general(wide(tjs), wide(ojs), contract, preferred_element_type=F32)
        acc_i[...] += lax.dot_general(wide(tis), wide(ois), contract, preferred_element_type=F32)

    blocks = pl_ref.shape[1] // width

    def step(block, carry):
        dots(jnp.maximum(block - 1, 0))
        compute(block)
        gather(jnp.minimum(block + 1, blocks - 1))
        return carry

    gather(0)
    rounds = len(distances)
    marks = [0] + [3 + 15 * k for k in range(rounds - 1)] + [blocks]
    for k in range(rounds):
        lax.fori_loop(marks[k], marks[k + 1], step, 0)
        if k + 1 < rounds:
            hear(k)
            tell(k + 1, distances[k + 1])
    for c in range(3):
        part[3 + c:4 + c, :] = -0.5 * jnp.sum(vacc[c], axis=0, keepdims=True)
    sums = jnp.sum(part[...], axis=1, keepdims=True)
    row = jnp.sum(jnp.where(sub == lane8, jnp.broadcast_to(sums, (8, L)), 0.0), axis=0, keepdims=True)
    src1[...] = row
    sum1[place] = src1[...]
    plane_copies = [
        copy(src1, sum1.at[place], send1.at[k], recv1.at[place], mate) for k, mate in enumerate(mates)]
    above = lax.rem(plane + 1, planes) * PLANE
    plane_copies += [
        copy(src1, prev1.at[place], send3.at[k], recv3.at[place], above + lax.rem(place + k, PLANE))
        for k in range(PLANE)]
    for item in plane_copies:
        item.start()
    dots(blocks - 1)
    tile_at = lambda k: acc_j[48 * k:48 * k + 24] + acc_j[48 * k + 24:48 * k + 48]
    near_force[0] = tile_at(1)
    near_force[1] = tile_at(2)
    far_force[...] = tile_at(3)
    near_copy = copy(near_force, near_in, force_send.at[0], force_recv.at[0], at(1))
    far_copy = copy(far_force, far_in, force_send.at[1], force_recv.at[1], at(2))
    far_copy.start()
    near_copy.start()
    tiles = [tile_at(0), near_force[0]]
    pad = jnp.zeros((24, L - half_c), F32)
    mi = [acc_i[48 * k:48 * k + 24] + acc_i[48 * k + 24:48 * k + 48] for k in range(2)]
    mi = [jnp.concatenate([v, pad], axis=1) for v in mi]
    hal1 = jnp.concatenate([halo_ref[...], jnp.full((1, L - fars), 4 * L, I32)], axis=1)
    oh_far = (jnp.broadcast_to(hal1, (clusters, L)) == iota((clusters, L), 0)).astype(F32).astype(BF16)

    hear(rounds - 1)
    for k in range(1, PLANE):
        other = lax.rem(place + k, PLANE)
        copy(src1, sum1.at[other], send1.at[k - 1], recv1.at[other], mates[k - 1]).wait_recv()
    row = sum1[0]
    for k in range(1, PLANE):
        row = row + sum1[k]
    src2[...] = row
    sum2[plane] = src2[...]
    column_copies = [
        copy(src2, sum2.at[plane], send2.at[k], recv2.at[plane], other) for k, other in enumerate(columns)]
    for item in column_copies:
        item.start()

    below = lax.rem(plane + planes - 1, planes)
    near_copy.wait()
    far_copy.wait()
    ff = far_in[...]
    f1 = ff.astype(BF16)
    r1 = ff - f1.astype(F32)
    f2 = r1.astype(BF16)
    f3 = (r1 - f2.astype(F32)).astype(BF16)
    far = sum(lax.dot_general(f, oh_far, (((1,), (1,)), ((), ())), preferred_element_type=F32) for f in (f3, f2, f1))
    tiles[0] = tiles[0] + far[:, 0:L]
    tiles[1] = tiles[1] + jnp.concatenate([far[:, L:], jnp.zeros((24, 2 * L - clusters), F32)], axis=1)
    back = [near_in[0], near_in[1]]
    pick = sub == (lane8 & 7)
    for c in range(3):
        for t in range(tiles_of):
            def window(tabs, slot, size):
                return take(tabs[slot // size][8 * c:8 * c + 8], slot % size + lane8 // 8)
            got = window(tiles, 16 * t, L) - window(mi, 16 * t, half_c) + window(back, half + 16 * t, L)
            force_ref[c:c + 1, t * L:(t + 1) * L] = jnp.sum(jnp.where(pick, got, 0.0), axis=0, keepdims=True)

    for item in plane_copies:
        item.wait_send()
    for k in range(PLANE):
        other = lax.rem(place + k, PLANE)
        copy(src1, prev1.at[other], send3.at[k], recv3.at[other], below * PLANE + other).wait_recv()
    row = prev1[0]
    for k in range(1, PLANE):
        row = row + prev1[k]
    sum2[below] = row
    for k, step_ in enumerate(steps):
        other = lax.rem(plane + planes - step_, planes)
        copy(src2, sum2.at[other], send2.at[k], recv2.at[other], columns[k]).wait_recv()
    row = sum2[0]
    for k in range(1, planes):
        row = row + sum2[k]
    row = jnp.broadcast_to(row, (8, L))
    one_of = [take(row, jnp.full((8, L), c, I32)) for c in range(6)]
    total = one_of[0] + one_of[1] + one_of[2]
    volume = box[0] * box[1] * box[2]
    ratio = 2.0 * total / (3.0 * (8 * clusters * domains) * thermal_scale_unit)
    coef = ext_ref[0] + reservoir_inertia_mass * (ratio - 1.0)
    for c in range(3):
        rate = ext_ref[1 + c] + barostat_gain * (
            one_of[c] - one_of[3 + c] - pressure_target * volume / 2.0
        ) / (total / 3.0)
        coef = jnp.where(sub == 1 + c, rate, coef)
    coef_ref[...] = coef
    for item in column_copies:
        item.wait_send()


def update_kernel(force_in, coef_ref, pos_ref, vel_ref, par_ref, force_ref, nvel_ref, npos_ref, coup_ref):
    coef = coef_ref[...]
    for k in range(4):
        coup_ref[k] = coef[k, 0]
    drag, grow = coef[0:1] + coef[1:4], 1.0 + time_step * coef[1:4]
    for t in range(pos_ref.shape[1] // L):
        cols = slice(t * L, (t + 1) * L)
        f, v = force_in[:, cols], vel_ref[:, cols]
        v = v + time_step * (f * par_ref[3:4, cols] - drag * v)
        force_ref[:, cols] = f
        nvel_ref[:, cols] = v
        npos_ref[:, cols] = pos_ref[:, cols] * grow + time_step * v


def on_device(
    positions,
    velocities,
    atom_params,
    pair_list,
    pair_count,
    exclusion,
    halo_far,
    box_lengths,
    extended_variables,
):
    domains = lax.axis_size("gx")
    planes = domains // PLANE
    atoms, fars = positions.shape[1], halo_far.shape[0]
    clusters, groups = atoms // 8, WIDTH // L
    vmem = pl.BlockSpec(memory_space=pltpu.VMEM)
    rows = jax.ShapeDtypeStruct((3, atoms), F32)
    dma = pltpu.SemaphoreType.DMA
    forces, coef = pl.pallas_call(
        functools.partial(step_kernel, domains),
        out_shape=(rows, jax.ShapeDtypeStruct((8, L), F32)),
        in_specs=[pl.BlockSpec(memory_space=pltpu.HBM)] * 9,
        out_specs=(vmem, vmem),
        scratch_shapes=[
            pltpu.SMEM((1,), I32),
            pltpu.SMEM((3,), F32),
            pltpu.SMEM((4,), F32),
            pltpu.VMEM((1, fars), I32),
            pltpu.VMEM((3, atoms), F32),
            pltpu.VMEM((3, atoms), F32),
            pltpu.VMEM((4, atoms), F32),
            pltpu.VMEM(pair_list.shape, I32),
            pltpu.VMEM(exclusion.shape, I32),
            pltpu.VMEM((6, 8, L), F32),
            pltpu.VMEM((3, 8, L), F32),
            pltpu.VMEM((6, 8, L), F32),
            pltpu.VMEM((3, 8, L), F32),
            pltpu.VMEM((2, 24, L), F32),
            pltpu.VMEM((24, L), F32),
            pltpu.VMEM((2, 24, L), F32),
            pltpu.VMEM((24, L), F32),
            pltpu.VMEM((8, L), F32),
            pltpu.VMEM((1, L), F32),
            pltpu.VMEM((1, L), F32),
            pltpu.VMEM((PLANE, 1, L), F32),
            pltpu.VMEM((PLANE, 1, L), F32),
            pltpu.VMEM((planes, 1, L), F32),
            pltpu.VMEM((6, 8, 2 * L), F32),
            pltpu.VMEM((4, 6, 8, L), F32),
            pltpu.VMEM((groups, 6, 16, L), F32),
            pltpu.VMEM((groups, 6, 8, L), F32),
            pltpu.VMEM((groups, 8, L), I32),
            pltpu.VMEM((groups, 6, 8, L), F32),
            pltpu.VMEM((192, L), F32),
            pltpu.VMEM((96, clusters // 2), F32),
            pltpu.VMEM((3, 8, L), F32),
            dma((9,)),
            dma((3,)),
            dma((3,)),
            dma((2,)),
            dma((2,)),
            dma((PLANE - 1,)),
            dma((PLANE,)),
            dma((PLANE,)),
            dma((PLANE,)),
            dma((planes - 2,)),
            dma((planes,)),
            pltpu.SemaphoreType.REGULAR((2 * planes.bit_length(),)),
        ],
        compiler_params=pltpu.CompilerParams(
            collective_id=0, has_side_effects=True, vmem_limit_bytes=50000 * 1024),
        name="force_step",
    )(pair_count, *[pltpu.with_memory_space_constraint(x, pltpu.HBM) for x in (box_lengths, extended_variables, halo_far[None], positions, velocities, atom_params,
      pair_list, exclusion)])
    return pl.pallas_call(
        update_kernel,
        out_shape=(rows, rows, rows, jax.ShapeDtypeStruct((4,), F32)),
        in_specs=[vmem] * 5,
        out_specs=(vmem, vmem, vmem, pl.BlockSpec(memory_space=pltpu.SMEM)),
        compiler_params=pltpu.CompilerParams(vmem_limit_bytes=8000 * 1024),
        name="update",
    )(forces, coef, positions, velocities, atom_params)


def solution(mesh):
    whole = ("rep", "gx")
    rows, flat = P(None, whole), P(whole)
    return jax.shard_map(
        on_device,
        mesh=mesh,
        in_specs=(rows, rows, rows, rows, flat, rows, flat, P("rep"), P("rep")),
        out_specs=(rows, rows, rows, P("rep")),
        check_vma=False,
    )
```

```python
import functools

import jax
import jax.numpy as jnp
from jax import lax
from jax.experimental import pallas as pl
from jax.experimental.pallas import tpu as pltpu
from jax.sharding import PartitionSpec as P

PLANE = 8
WIDTH = 512
MESH = pl.DeviceIdType.MESH

time_step = 0.25
thermal_scale_unit = 2.0
reservoir_inertia_mass = 4.0
barostat_gain = 0.1
pressure_target = 1.0

RT = 1.0 / 1331.0
L = 128
F32, BF16, I16, I32 = jnp.float32, jnp.bfloat16, jnp.int16, jnp.int32


def take(x, idx):
    dn = lax.GatherDimensionNumbers(offset_dims=(), collapsed_slice_dims=(1,), start_index_map=(1,),
                                    operand_batching_dims=(0,), start_indices_batching_dims=(0,))
    return lax.gather(x, idx[:, :, None], dn, (1, 1), mode=lax.GatherScatterMode.PROMISE_IN_BOUNDS)


def iota(shape, dim):
    return lax.broadcasted_iota(I32, shape, dim)


def to_cluster_rows(row, clusters):
    lane, sub = iota((8, L), 1), iota((8, L), 0)
    idx = 8 * (lane % 16) + sub
    part = lane // 16
    tiles = []
    for t in range((clusters + L - 1) // L):
        out = None
        for u in range(8):
            start = (8 * t + u) * L
            if start >= 8 * clusters:
                break
            got = take(row(start), idx)
            out = got if out is None else jnp.where(part == u, got, out)
        tiles.append(out)
    return tiles


def step_kernel(
    domains, count_in, box_in, ext_in, halo_in, pos_in, vel_in, par_in, pl_in, ex_in,
    force_ref, coef_ref,
    count_ref, box_ref, ext_ref, halo_ref, pos_ref, vel_ref, par_ref, pl_ref, ex_ref,
    near_out, mix_out, far_out, mix_in, near_force, far_force, near_in, far_in,
    part, src1, src2, sum1, prev1, sum2,
    tab_i, tab_j, jd, ri, wd, fs, acc_j, acc_i, vacc,
    load_sem, halo_send, halo_recv, force_send, force_recv, send1, recv1, send3, recv3, send2, recv2, relay,
):
    planes = domains // PLANE
    me = lax.axis_index("gx")
    place, plane = lax.rem(me, PLANE), lax.div(me, PLANE)
    at = lambda shift: lax.rem(me + domains + shift, domains)
    column = lambda shift: lax.rem(plane + planes + shift, planes) * PLANE + place
    mates = [plane * PLANE + lax.rem(place + k, PLANE) for k in range(1, PLANE)]
    steps = sorted(range(2, planes), key=lambda k: min(k, planes - k))
    columns = [column(k) for k in steps]

    barrier = pltpu.get_barrier_semaphore()
    greeted = [at(2), at(1), at(-1), at(-2), column(1), column(-1)] + mates
    for other in greeted:
        pl.semaphore_signal(barrier, inc=1, device_id={"gx": other}, device_id_type=MESH)

    loads = [
        pltpu.make_async_copy(src, dst, load_sem.at[k])
        for k, (src, dst) in enumerate((
            (pos_in, pos_ref), (par_in, par_ref), (halo_in, halo_ref), (box_in, box_ref), (vel_in, vel_ref),
            (count_in, count_ref), (ext_in, ext_ref), (pl_in, pl_ref), (ex_in, ex_ref),
        ))
    ]
    for item in loads:
        item.start()

    def copy(src, dst, send, recv, other):
        return pltpu.make_async_remote_copy(
            src_ref=src, dst_ref=dst, send_sem=send, recv_sem=recv, device_id={"gx": other}, device_id_type=MESH
        )

    halo_copies = [
        copy(near_out, tab_j.at[2], halo_send.at[0], halo_recv.at[0], at(-1)),
        copy(mix_out, mix_in, halo_send.at[1], halo_recv.at[1], at(-1)),
        copy(far_out, tab_j.at[3], halo_send.at[2], halo_recv.at[2], at(-2)),
    ]
    for item in loads[:4]:
        item.wait()

    clusters = pos_ref.shape[1] // 8
    fars = halo_ref.shape[1]
    width = fs.shape[0] * L
    box = [box_ref[c] for c in range(3)]

    def row_of(c):
        def row(start):
            ref, r = (pos_ref, c) if c < 3 else (par_ref, c - 3)
            return jnp.broadcast_to(ref[pl.ds(r, 1), pl.ds(start, L)], (8, L))
        return row

    lane8 = iota((8, L), 1)
    tiles_of = clusters // 16
    half = clusters - L
    scales = (1.0, 1.0, 1.0, 1.0, 6.0, 12.0)
    hal = jnp.concatenate(
        [jnp.broadcast_to(halo_ref[...], (8, fars)), jnp.zeros((8, L - fars), I32)], axis=1)
    lifts = [jnp.where(me < k, box[0], 0.0) for k in (1, 2)]
    heads = []
    for c in range(6):
        own = to_cluster_rows(row_of(c), clusters)
        for t in range(2):
            tab_i[c, :, t * L:(t + 1) * L] = own[t] * scales[c] if scales[c] != 1.0 else own[t]
            tab_j[t, c] = own[t]
        far = jnp.where(hal >= L, take(own[1], hal & (L - 1)), take(own[0], hal & (L - 1)))
        far_out[c] = far + lifts[1] if c == 0 else far
        if c == 0:
            own = [v + lifts[0] for v in own]
        rot0, rot1 = pltpu.roll(own[0], half, 1), pltpu.roll(own[1], half, 1)
        near_out[c] = jnp.where(lane8 < half, rot0, rot1)
        if c < 3:
            heads.append(rot0)
        else:
            mix_out[c - 3] = jnp.where(lane8 < half, own[0], heads[c - 3])
    pl.semaphore_wait(barrier, len(greeted))
    for item in (halo_copies[2], halo_copies[0], halo_copies[1]):
        item.start()

    def tell(round_, distance):
        for side in (0, 1):
            pl.semaphore_signal(
                relay.at[2 * round_ + side], inc=1,
                device_id={"gx": column(distance if side else -distance)}, device_id_type=MESH)

    def hear(round_):
        for side in (0, 1):
            pl.semaphore_wait(relay.at[2 * round_ + side], 1)

    distances = []
    while 2 ** (len(distances) + 1) < planes:
        distances.append(2 ** len(distances))
    tell(0, distances[0])

    for item in loads[4:]:
        item.wait()
    part[...] = jnp.zeros_like(part)
    kin = None
    for t in range(tiles_of):
        cols = slice(t * L, (t + 1) * L)
        term = vel_ref[:, cols] * vel_ref[:, cols] / par_ref[3:4, cols]
        kin = term if kin is None else kin + term
    part[0:3, :] = 0.5 * kin
    acc_j[...] = jnp.zeros_like(acc_j)
    acc_i[...] = jnp.zeros_like(acc_i)
    vacc[...] = jnp.zeros_like(vacc)
    fs[...] = jnp.zeros_like(fs)

    for item in halo_copies:
        item.wait()
    for c in range(3):
        mixed = mix_in[c]
        tab_j[1, c] = jnp.where(lane8 < half, tab_j[1, c], mixed)
        tab_j[1, c + 3] = jnp.where(lane8 < half, tab_j[1, c + 3], pltpu.roll(mixed, half, 1))

    sub = iota((8, L), 0)
    count = count_ref[0]
    shift0 = 8 * (sub % 2)
    bits = [jnp.left_shift(1, shift0 + ((sub + m) & 7)) for m in range(8)]
    one16 = jnp.ones((16, L), BF16)
    zero16 = jnp.zeros((16, L), BF16)

    groups = width // L
    bases = [(iota((16, L), 0) + 16 * r).astype(I16) for r in range(L // 16)]

    def gather(block):
        for g in range(groups):
            first = block * width + g * L
            cols = pl.ds(pl.multiple_of(first, L), L)
            ib = jnp.broadcast_to(pl_ref[pl.ds(0, 1), cols], (8, L))
            jb = jnp.broadcast_to(pl_ref[pl.ds(1, 1), cols], (8, L))
            sb = jnp.broadcast_to(pl_ref[pl.ds(2, 1), cols], (8, L))
            usable = lane8 < count - first
            w = [jnp.broadcast_to(ex_ref[pl.ds(k, 1), cols], (8, L)) for k in range(4)]
            words = jnp.where(sub < 4, jnp.where(sub < 2, w[0], w[1]), jnp.where(sub < 6, w[2], w[3]))
            wd[g] = jnp.where(usable, words, 0)
            above_y, below_y = sb >= 6, sb < 3
            s3 = sb - jnp.where(above_y, 6, jnp.where(below_y, 0, 3))
            il, ih = ib & (L - 1), ib >= L
            jl, jh, jm = jb & (L - 1), jb >= 2 * L, (jb & L) != 0
            for c in range(6):
                v = jnp.where(ih, take(tab_i[c, :, L:2 * L], il), take(tab_i[c, :, 0:L], il))
                if c in (1, 2):
                    v = v - jnp.where(above_y if c == 1 else s3 == 2, box[c], 0.0)
                ri[g, c] = v
            for c in range(6):
                q = [take(tab_j[t, c], jl) for t in range(4)]
                v = jnp.where(jh, jnp.where(jm, q[3], q[2]), jnp.where(jm, q[1], q[0]))
                if c in (1, 2):
                    v = v - jnp.where(below_y if c == 1 else s3 == 0, box[c], 0.0)
                jd[g, c, 0:8, :] = v
                jd[g, c, 8:16, :] = v

    def split(fs):
        hi = [f.astype(BF16).astype(F32) for f in fs]
        lo = [f - h for f, h in zip(fs, hi)]
        return jnp.concatenate(hi + lo, axis=0).astype(BF16)

    def compute(block):
        for g in range(groups):
            xi, yi, zi, qi, ei, bi = [ri[g, c] for c in range(6)]
            words = wd[g]
            fi, fj = [None] * 3, [None] * 3
            for m in range(7, -1, -1):
                xj, yj, zj, qj, ej, bj = [jd[g, c, m:m + 8, :] for c in range(6)]
                d = (xj - xi, yj - yi, zj - zi)
                r2 = d[0] * d[0] + d[1] * d[1] + d[2] * d[2]
                inv = lax.rsqrt(r2)
                inv2 = inv * inv
                inv3 = inv * inv2
                inv6 = inv3 * inv3
                s = qi * qj * (inv3 - RT) + (bi * bj * inv6 - ei * ej) * (inv6 * inv2)
                s = jnp.where((words & bits[m]) != 0, s, 0.0)
                for c in range(3):
                    f = s * d[c]
                    fi[c] = f if fi[c] is None else fi[c] + f
                    fj[c] = f if fj[c] is None else pltpu.roll(fj[c], 1, 0) + f
            for c, v in enumerate((xi, yi, zi)):
                origin = jnp.broadcast_to(ri[g, c, 0:1, :], (8, L))
                vacc[c] += fj[c] * (jd[g, c, 0:8, :] - origin) - fi[c] * (v - origin)
            for c in range(3):
                fs[g, c] = fj[c]
                fs[g, 3 + c] = fi[c]

    half_c = clusters // 2

    def dots(block):
        tjs, tis, ojs, ois = [], [], [], []
        for g in range(groups):
            cols = pl.ds(pl.multiple_of(block * width + g * L, L), L)
            j16 = jnp.broadcast_to(pl_ref[pl.ds(1, 1), cols], (16, L)).astype(I16)
            i16 = jnp.broadcast_to(pl_ref[pl.ds(0, 1), cols], (16, L)).astype(I16)
            tj = split([fs[g, c] for c in range(3)])
            ti = split([fs[g, 3 + c] for c in range(3)])
            parts = lambda t: [t[16 * r:16 * r + 16] for r in range(3)]
            which = j16 & (3 * L)
            tjs.append(jnp.concatenate(
                [jnp.where(which == k * L, p, zero16) for k in range(4) for p in parts(tj)], axis=0))
            later = i16 >= half_c
            tis.append(jnp.concatenate(
                [jnp.where(later, zero16, p) for p in parts(ti)] + [jnp.where(later, p, zero16) for p in parts(ti)], axis=0))
            j16 = j16 & (L - 1)
            i16 = jnp.where(later, i16 - half_c, i16)
            ojs.append(jnp.concatenate([jnp.where(bases[r] == j16, one16, zero16) for r in range(L // 16)], axis=0))
            ois.append(jnp.concatenate([jnp.where(bases[r] == i16, one16, zero16) for r in range(half_c // 16)], axis=0))
        contract = (((1,), (1,)), ((), ()))
        wide = lambda xs: jnp.concatenate(xs, axis=1)
        acc_j[...] += lax.dot_general(wide(tjs), wide(ojs), contract, preferred_element_type=F32)
        acc_i[...] += lax.dot_general(wide(tis), wide(ois), contract, preferred_element_type=F32)

    blocks = pl_ref.shape[1] // width

    def step(block, carry):
        dots(jnp.maximum(block - 1, 0))
        compute(block)
        gather(jnp.minimum(block + 1, blocks - 1))
        return carry

    gather(0)
    rounds = len(distances)
    marks = [0] + [3 + 15 * k for k in range(rounds - 1)] + [blocks]
    for k in range(rounds):
        lax.fori_loop(marks[k], marks[k + 1], step, 0)
        if k + 1 < rounds:
            hear(k)
            tell(k + 1, distances[k + 1])
    for c in range(3):
        part[3 + c:4 + c, :] = -0.5 * jnp.sum(vacc[c], axis=0, keepdims=True)
    sums = jnp.sum(part[...], axis=1, keepdims=True)
    row = jnp.sum(jnp.where(sub == lane8, jnp.broadcast_to(sums, (8, L)), 0.0), axis=0, keepdims=True)
    src1[...] = row
    sum1[place] = src1[...]
    plane_copies = [
        copy(src1, sum1.at[place], send1.at[k], recv1.at[place], mate) for k, mate in enumerate(mates)]
    above = lax.rem(plane + 1, planes) * PLANE
    plane_copies += [
        copy(src1, prev1.at[place], send3.at[k], recv3.at[place], above + lax.rem(place + k, PLANE))
        for k in range(PLANE)]
    for item in plane_copies:
        item.start()
    dots(blocks - 1)
    tile_at = lambda k: acc_j[48 * k:48 * k + 24] + acc_j[48 * k + 24:48 * k + 48]
    near_force[0] = tile_at(1)
    near_force[1] = tile_at(2)
    far_force[...] = tile_at(3)
    near_copy = copy(near_force, near_in, force_send.at[0], force_recv.at[0], at(1))
    far_copy = copy(far_force, far_in, force_send.at[1], force_recv.at[1], at(2))
    far_copy.start()
    near_copy.start()
    tiles = [tile_at(0), near_force[0]]
    pad = jnp.zeros((24, L - half_c), F32)
    mi = [acc_i[48 * k:48 * k + 24] + acc_i[48 * k + 24:48 * k + 48] for k in range(2)]
    mi = [jnp.concatenate([v, pad], axis=1) for v in mi]
    hal1 = jnp.concatenate([halo_ref[...], jnp.full((1, L - fars), 4 * L, I32)], axis=1)
    oh_far = (jnp.broadcast_to(hal1, (clusters, L)) == iota((clusters, L), 0)).astype(F32).astype(BF16)

    hear(rounds - 1)
    for k in range(1, PLANE):
        other = lax.rem(place + k, PLANE)
        copy(src1, sum1.at[other], send1.at[k - 1], recv1.at[other], mates[k - 1]).wait_recv()
    row = sum1[0]
    for k in range(1, PLANE):
        row = row + sum1[k]
    src2[...] = row
    sum2[plane] = src2[...]
    column_copies = [
        copy(src2, sum2.at[plane], send2.at[k], recv2.at[plane], other) for k, other in enumerate(columns)]
    for item in column_copies:
        item.start()

    below = lax.rem(plane + planes - 1, planes)
    near_copy.wait()
    far_copy.wait()
    ff = far_in[...]
    f1 = ff.astype(BF16)
    r1 = ff - f1.astype(F32)
    f2 = r1.astype(BF16)
    f3 = (r1 - f2.astype(F32)).astype(BF16)
    far = sum(lax.dot_general(f, oh_far, (((1,), (1,)), ((), ())), preferred_element_type=F32) for f in (f3, f2, f1))
    tiles[0] = tiles[0] + far[:, 0:L]
    tiles[1] = tiles[1] + jnp.concatenate([far[:, L:], jnp.zeros((24, 2 * L - clusters), F32)], axis=1)
    back = [near_in[0], near_in[1]]
    pick = sub == (lane8 & 7)
    for c in range(3):
        for t in range(tiles_of):
            def window(tabs, slot, size):
                return take(tabs[slot // size][8 * c:8 * c + 8], slot % size + lane8 // 8)
            got = window(tiles, 16 * t, L) - window(mi, 16 * t, half_c) + window(back, half + 16 * t, L)
            force_ref[c:c + 1, t * L:(t + 1) * L] = jnp.sum(jnp.where(pick, got, 0.0), axis=0, keepdims=True)

    for item in plane_copies:
        item.wait_send()
    for k in range(PLANE):
        other = lax.rem(place + k, PLANE)
        copy(src1, prev1.at[other], send3.at[k], recv3.at[other], below * PLANE + other).wait_recv()
    row = prev1[0]
    for k in range(1, PLANE):
        row = row + prev1[k]
    sum2[below] = row
    for k, step_ in enumerate(steps):
        other = lax.rem(plane + planes - step_, planes)
        copy(src2, sum2.at[other], send2.at[k], recv2.at[other], columns[k]).wait_recv()
    row = sum2[0]
    for k in range(1, planes):
        row = row + sum2[k]
    row = jnp.broadcast_to(row, (8, L))
    one_of = [take(row, jnp.full((8, L), c, I32)) for c in range(6)]
    total = one_of[0] + one_of[1] + one_of[2]
    volume = box[0] * box[1] * box[2]
    ratio = 2.0 * total / (3.0 * (8 * clusters * domains) * thermal_scale_unit)
    coef = ext_ref[0] + reservoir_inertia_mass * (ratio - 1.0)
    for c in range(3):
        rate = ext_ref[1 + c] + barostat_gain * (
            one_of[c] - one_of[3 + c] - pressure_target * volume / 2.0
        ) / (total / 3.0)
        coef = jnp.where(sub == 1 + c, rate, coef)
    coef_ref[...] = coef
    for item in column_copies:
        item.wait_send()


def update_kernel(force_in, coef_ref, pos_ref, vel_ref, par_ref, force_ref, nvel_ref, npos_ref, coup_ref):
    coef = coef_ref[...]
    for k in range(4):
        coup_ref[k] = coef[k, 0]
    drag, grow = coef[0:1] + coef[1:4], 1.0 + time_step * coef[1:4]
    for t in range(pos_ref.shape[1] // L):
        cols = slice(t * L, (t + 1) * L)
        f, v = force_in[:, cols], vel_ref[:, cols]
        v = v + time_step * (f * par_ref[3:4, cols] - drag * v)
        force_ref[:, cols] = f
        nvel_ref[:, cols] = v
        npos_ref[:, cols] = pos_ref[:, cols] * grow + time_step * v


def on_device(
    positions,
    velocities,
    atom_params,
    pair_list,
    pair_count,
    exclusion,
    halo_far,
    box_lengths,
    extended_variables,
):
    domains = lax.axis_size("gx")
    planes = domains // PLANE
    atoms, fars = positions.shape[1], halo_far.shape[0]
    clusters, groups = atoms // 8, WIDTH // L
    vmem = pl.BlockSpec(memory_space=pltpu.VMEM)
    rows = jax.ShapeDtypeStruct((3, atoms), F32)
    dma = pltpu.SemaphoreType.DMA
    forces, coef = pl.pallas_call(
        functools.partial(step_kernel, domains),
        out_shape=(rows, jax.ShapeDtypeStruct((8, L), F32)),
        in_specs=[pl.BlockSpec(memory_space=pltpu.HBM)] * 9,
        out_specs=(vmem, vmem),
        scratch_shapes=[
            pltpu.SMEM((1,), I32),
            pltpu.SMEM((3,), F32),
            pltpu.SMEM((4,), F32),
            pltpu.VMEM((1, fars), I32),
            pltpu.VMEM((3, atoms), F32),
            pltpu.VMEM((3, atoms), F32),
            pltpu.VMEM((4, atoms), F32),
            pltpu.VMEM(pair_list.shape, I32),
            pltpu.VMEM(exclusion.shape, I32),
            pltpu.VMEM((6, 8, L), F32),
            pltpu.VMEM((3, 8, L), F32),
            pltpu.VMEM((6, 8, L), F32),
            pltpu.VMEM((3, 8, L), F32),
            pltpu.VMEM((2, 24, L), F32),
            pltpu.VMEM((24, L), F32),
            pltpu.VMEM((2, 24, L), F32),
            pltpu.VMEM((24, L), F32),
            pltpu.VMEM((8, L), F32),
            pltpu.VMEM((1, L), F32),
            pltpu.VMEM((1, L), F32),
            pltpu.VMEM((PLANE, 1, L), F32),
            pltpu.VMEM((PLANE, 1, L), F32),
            pltpu.VMEM((planes, 1, L), F32),
            pltpu.VMEM((6, 8, 2 * L), F32),
            pltpu.VMEM((4, 6, 8, L), F32),
            pltpu.VMEM((groups, 6, 16, L), F32),
            pltpu.VMEM((groups, 6, 8, L), F32),
            pltpu.VMEM((groups, 8, L), I32),
            pltpu.VMEM((groups, 6, 8, L), F32),
            pltpu.VMEM((192, L), F32),
            pltpu.VMEM((96, clusters // 2), F32),
            pltpu.VMEM((3, 8, L), F32),
            dma((9,)),
            dma((3,)),
            dma((3,)),
            dma((2,)),
            dma((2,)),
            dma((PLANE - 1,)),
            dma((PLANE,)),
            dma((PLANE,)),
            dma((PLANE,)),
            dma((planes - 2,)),
            dma((planes,)),
            pltpu.SemaphoreType.REGULAR((2 * planes.bit_length(),)),
        ],
        compiler_params=pltpu.CompilerParams(
            collective_id=0, has_side_effects=True, vmem_limit_bytes=50000 * 1024),
        name="force_step",
    )(pair_count, *[pltpu.with_memory_space_constraint(x, pltpu.HBM) for x in (box_lengths, extended_variables, halo_far[None], positions, velocities, atom_params,
      pair_list, exclusion)])
    return pl.pallas_call(
        update_kernel,
        out_shape=(rows, rows, rows, jax.ShapeDtypeStruct((4,), F32)),
        in_specs=[vmem] * 5,
        out_specs=(vmem, vmem, vmem, pl.BlockSpec(memory_space=pltpu.SMEM)),
        compiler_params=pltpu.CompilerParams(vmem_limit_bytes=8000 * 1024),
        name="update",
    )(forces, coef, positions, velocities, atom_params)


def solution(mesh):
    whole = ("rep", "gx")
    rows, flat = P(None, whole), P(whole)
    return jax.shard_map(
        on_device,
        mesh=mesh,
        in_specs=(rows, rows, rows, rows, flat, rows, flat, P("rep"), P("rep")),
        out_specs=(rows, rows, rows, P("rep")),
        check_vma=False,
    )
```

```python
import functools

import jax
import jax.numpy as jnp
from jax import lax
from jax.experimental import pallas as pl
from jax.experimental.pallas import tpu as pltpu
from jax.sharding import PartitionSpec as P

PLANE = 8
WIDTH = 512
MESH = pl.DeviceIdType.MESH

time_step = 0.25
thermal_scale_unit = 2.0
reservoir_inertia_mass = 4.0
barostat_gain = 0.1
pressure_target = 1.0

RT = 1.0 / 1331.0
L = 128
F32, BF16, I16, I32 = jnp.float32, jnp.bfloat16, jnp.int16, jnp.int32


def take(x, idx):
    dn = lax.GatherDimensionNumbers(offset_dims=(), collapsed_slice_dims=(1,), start_index_map=(1,),
                                    operand_batching_dims=(0,), start_indices_batching_dims=(0,))
    return lax.gather(x, idx[:, :, None], dn, (1, 1), mode=lax.GatherScatterMode.PROMISE_IN_BOUNDS)


def iota(shape, dim):
    return lax.broadcasted_iota(I32, shape, dim)


def to_cluster_rows(row, clusters):
    lane, sub = iota((8, L), 1), iota((8, L), 0)
    idx = 8 * (lane % 16) + sub
    part = lane // 16
    tiles = []
    for t in range((clusters + L - 1) // L):
        out = None
        for u in range(8):
            start = (8 * t + u) * L
            if start >= 8 * clusters:
                break
            got = take(row(start), idx)
            out = got if out is None else jnp.where(part == u, got, out)
        tiles.append(out)
    return tiles


def step_kernel(
    domains, count_in, box_in, ext_in, halo_in, pos_in, vel_in, par_in, pl_in, ex_in,
    force_ref, coef_ref,
    count_ref, box_ref, ext_ref, halo_ref, pos_ref, vel_ref, par_ref, pl_ref, ex_ref,
    near_out, mix_out, far_out, mix_in, near_force, far_force, near_in, far_in,
    part, src1, src2, sum1, prev1, sum2,
    tab_i, tab_j, jd, ri, wd, fs, acc_j, acc_i, vacc,
    load_sem, halo_send, halo_recv, force_send, force_recv, send1, recv1, send3, recv3, send2, recv2, relay,
):
    planes = domains // PLANE
    me = lax.axis_index("gx")
    place, plane = lax.rem(me, PLANE), lax.div(me, PLANE)
    at = lambda shift: lax.rem(me + domains + shift, domains)
    column = lambda shift: lax.rem(plane + planes + shift, planes) * PLANE + place
    mates = [plane * PLANE + lax.rem(place + k, PLANE) for k in range(1, PLANE)]
    steps = sorted(range(2, planes), key=lambda k: min(k, planes - k))
    columns = [column(k) for k in steps]

    barrier = pltpu.get_barrier_semaphore()
    greeted = [at(2), at(1), at(-1), at(-2), column(1), column(-1)] + mates
    for other in greeted:
        pl.semaphore_signal(barrier, inc=1, device_id={"gx": other}, device_id_type=MESH)

    loads = [
        pltpu.make_async_copy(src, dst, load_sem.at[k])
        for k, (src, dst) in enumerate((
            (pos_in, pos_ref), (par_in, par_ref), (halo_in, halo_ref), (box_in, box_ref), (vel_in, vel_ref),
            (count_in, count_ref), (ext_in, ext_ref), (pl_in, pl_ref), (ex_in, ex_ref),
        ))
    ]
    for item in loads:
        item.start()

    def copy(src, dst, send, recv, other):
        return pltpu.make_async_remote_copy(
            src_ref=src, dst_ref=dst, send_sem=send, recv_sem=recv, device_id={"gx": other}, device_id_type=MESH
        )

    halo_copies = [
        copy(near_out, tab_j.at[2], halo_send.at[0], halo_recv.at[0], at(-1)),
        copy(mix_out, mix_in, halo_send.at[1], halo_recv.at[1], at(-1)),
        copy(far_out, tab_j.at[3], halo_send.at[2], halo_recv.at[2], at(-2)),
    ]
    for item in loads[:4]:
        item.wait()

    clusters = pos_ref.shape[1] // 8
    fars = halo_ref.shape[1]
    width = fs.shape[0] * L
    box = [box_ref[c] for c in range(3)]

    def row_of(c):
        def row(start):
            ref, r = (pos_ref, c) if c < 3 else (par_ref, c - 3)
            return jnp.broadcast_to(ref[pl.ds(r, 1), pl.ds(start, L)], (8, L))
        return row

    lane8 = iota((8, L), 1)
    tiles_of = clusters // 16
    half = clusters - L
    scales = (1.0, 1.0, 1.0, 1.0, 6.0, 12.0)
    hal = jnp.concatenate(
        [jnp.broadcast_to(halo_ref[...], (8, fars)), jnp.zeros((8, L - fars), I32)], axis=1)
    lifts = [jnp.where(me < k, box[0], 0.0) for k in (1, 2)]
    heads = []
    for c in range(6):
        own = to_cluster_rows(row_of(c), clusters)
        for t in range(2):
            tab_i[c, :, t * L:(t + 1) * L] = own[t] * scales[c] if scales[c] != 1.0 else own[t]
            tab_j[t, c] = own[t]
        far = jnp.where(hal >= L, take(own[1], hal & (L - 1)), take(own[0], hal & (L - 1)))
        far_out[c] = far + lifts[1] if c == 0 else far
        if c == 0:
            own = [v + lifts[0] for v in own]
        rot0, rot1 = pltpu.roll(own[0], half, 1), pltpu.roll(own[1], half, 1)
        near_out[c] = jnp.where(lane8 < half, rot0, rot1)
        if c < 3:
            heads.append(rot0)
        else:
            mix_out[c - 3] = jnp.where(lane8 < half, own[0], heads[c - 3])
    pl.semaphore_wait(barrier, len(greeted))
    for item in (halo_copies[2], halo_copies[0], halo_copies[1]):
        item.start()

    def tell(round_, distance):
        for side in (0, 1):
            pl.semaphore_signal(
                relay.at[2 * round_ + side], inc=1,
                device_id={"gx": column(distance if side else -distance)}, device_id_type=MESH)

    def hear(round_):
        for side in (0, 1):
            pl.semaphore_wait(relay.at[2 * round_ + side], 1)

    distances = []
    while 2 ** (len(distances) + 1) < planes:
        distances.append(2 ** len(distances))
    tell(0, distances[0])

    for item in loads[4:]:
        item.wait()
    part[...] = jnp.zeros_like(part)
    kin = None
    for t in range(tiles_of):
        cols = slice(t * L, (t + 1) * L)
        term = vel_ref[:, cols] * vel_ref[:, cols] / par_ref[3:4, cols]
        kin = term if kin is None else kin + term
    part[0:3, :] = 0.5 * kin
    acc_j[...] = jnp.zeros_like(acc_j)
    acc_i[...] = jnp.zeros_like(acc_i)
    vacc[...] = jnp.zeros_like(vacc)
    fs[...] = jnp.zeros_like(fs)

    for item in halo_copies:
        item.wait()
    for c in range(3):
        mixed = mix_in[c]
        tab_j[1, c] = jnp.where(lane8 < half, tab_j[1, c], mixed)
        tab_j[1, c + 3] = jnp.where(lane8 < half, tab_j[1, c + 3], pltpu.roll(mixed, half, 1))

    sub = iota((8, L), 0)
    count = count_ref[0]
    shift0 = 8 * (sub % 2)
    bits = [jnp.left_shift(1, shift0 + ((sub + m) & 7)) for m in range(8)]
    one16 = jnp.ones((16, L), BF16)
    zero16 = jnp.zeros((16, L), BF16)

    groups = width // L
    bases = [(iota((16, L), 0) + 16 * r).astype(I16) for r in range(L // 16)]

    def gather(block):
        for g in range(groups):
            first = block * width + g * L
            cols = pl.ds(pl.multiple_of(first, L), L)
            ib = jnp.broadcast_to(pl_ref[pl.ds(0, 1), cols], (8, L))
            jb = jnp.broadcast_to(pl_ref[pl.ds(1, 1), cols], (8, L))
            sb = jnp.broadcast_to(pl_ref[pl.ds(2, 1), cols], (8, L))
            usable = lane8 < count - first
            w = [jnp.broadcast_to(ex_ref[pl.ds(k, 1), cols], (8, L)) for k in range(4)]
            words = jnp.where(sub < 4, jnp.where(sub < 2, w[0], w[1]), jnp.where(sub < 6, w[2], w[3]))
            wd[g] = jnp.where(usable, words, 0)
            above_y, below_y = sb >= 6, sb < 3
            s3 = sb - jnp.where(above_y, 6, jnp.where(below_y, 0, 3))
            il, ih = ib & (L - 1), ib >= L
            jl, jh, jm = jb & (L - 1), jb >= 2 * L, (jb & L) != 0
            for c in range(6):
                v = jnp.where(ih, take(tab_i[c, :, L:2 * L], il), take(tab_i[c, :, 0:L], il))
                if c in (1, 2):
                    v = v - jnp.where(above_y if c == 1 else s3 == 2, box[c], 0.0)
                ri[g, c] = v
            for c in range(6):
                q = [take(tab_j[t, c], jl) for t in range(4)]
                v = jnp.where(jh, jnp.where(jm, q[3], q[2]), jnp.where(jm, q[1], q[0]))
                if c in (1, 2):
                    v = v - jnp.where(below_y if c == 1 else s3 == 0, box[c], 0.0)
                jd[g, c, 0:8, :] = v
                jd[g, c, 8:16, :] = v

    def split(fs):
        hi = [f.astype(BF16).astype(F32) for f in fs]
        lo = [f - h for f, h in zip(fs, hi)]
        return jnp.concatenate(hi + lo, axis=0).astype(BF16)

    def compute(block):
        for g in range(groups):
            xi, yi, zi, qi, ei, bi = [ri[g, c] for c in range(6)]
            words = wd[g]
            fi, fj = [None] * 3, [None] * 3
            for m in range(7, -1, -1):
                xj, yj, zj, qj, ej, bj = [jd[g, c, m:m + 8, :] for c in range(6)]
                d = (xj - xi, yj - yi, zj - zi)
                r2 = d[0] * d[0] + d[1] * d[1] + d[2] * d[2]
                inv = lax.rsqrt(r2)
                inv2 = inv * inv
                inv3 = inv * inv2
                inv6 = inv3 * inv3
                s = qi * qj * (inv3 - RT) + (bi * bj * inv6 - ei * ej) * (inv6 * inv2)
                s = jnp.where((words & bits[m]) != 0, s, 0.0)
                for c in range(3):
                    f = s * d[c]
                    fi[c] = f if fi[c] is None else fi[c] + f
                    fj[c] = f if fj[c] is None else pltpu.roll(fj[c], 1, 0) + f
            for c, v in enumerate((xi, yi, zi)):
                origin = jnp.broadcast_to(ri[g, c, 0:1, :], (8, L))
                vacc[c] += fj[c] * (jd[g, c, 0:8, :] - origin) - fi[c] * (v - origin)
            for c in range(3):
                fs[g, c] = fj[c]
                fs[g, 3 + c] = fi[c]

    half_c = clusters // 2

    def dots(block):
        tjs, tis, ojs, ois = [], [], [], []
        for g in range(groups):
            cols = pl.ds(pl.multiple_of(block * width + g * L, L), L)
            j16 = jnp.broadcast_to(pl_ref[pl.ds(1, 1), cols], (16, L)).astype(I16)
            i16 = jnp.broadcast_to(pl_ref[pl.ds(0, 1), cols], (16, L)).astype(I16)
            tj = split([fs[g, c] for c in range(3)])
            ti = split([fs[g, 3 + c] for c in range(3)])
            parts = lambda t: [t[16 * r:16 * r + 16] for r in range(3)]
            which = j16 & (3 * L)
            tjs.append(jnp.concatenate(
                [jnp.where(which == k * L, p, zero16) for k in range(4) for p in parts(tj)], axis=0))
            later = i16 >= half_c
            tis.append(jnp.concatenate(
                [jnp.where(later, zero16, p) for p in parts(ti)] + [jnp.where(later, p, zero16) for p in parts(ti)], axis=0))
            j16 = j16 & (L - 1)
            i16 = jnp.where(later, i16 - half_c, i16)
            ojs.append(jnp.concatenate([jnp.where(bases[r] == j16, one16, zero16) for r in range(L // 16)], axis=0))
            ois.append(jnp.concatenate([jnp.where(bases[r] == i16, one16, zero16) for r in range(half_c // 16)], axis=0))
        contract = (((1,), (1,)), ((), ()))
        wide = lambda xs: jnp.concatenate(xs, axis=1)
        acc_j[...] += lax.dot_general(wide(tjs), wide(ojs), contract, preferred_element_type=F32)
        acc_i[...] += lax.dot_general(wide(tis), wide(ois), contract, preferred_element_type=F32)

    blocks = pl_ref.shape[1] // width

    def step(block, carry):
        dots(jnp.maximum(block - 1, 0))
        compute(block)
        gather(jnp.minimum(block + 1, blocks - 1))
        return carry

    gather(0)
    rounds = len(distances)
    marks = [0] + [3 + 15 * k for k in range(rounds - 1)] + [blocks]
    for k in range(rounds):
        lax.fori_loop(marks[k], marks[k + 1], step, 0)
        if k + 1 < rounds:
            hear(k)
            tell(k + 1, distances[k + 1])
    for c in range(3):
        part[3 + c:4 + c, :] = -0.5 * jnp.sum(vacc[c], axis=0, keepdims=True)
    sums = jnp.sum(part[...], axis=1, keepdims=True)
    row = jnp.sum(jnp.where(sub == lane8, jnp.broadcast_to(sums, (8, L)), 0.0), axis=0, keepdims=True)
    src1[...] = row
    sum1[place] = src1[...]
    plane_copies = [
        copy(src1, sum1.at[place], send1.at[k], recv1.at[place], mate) for k, mate in enumerate(mates)]
    above = lax.rem(plane + 1, planes) * PLANE
    plane_copies += [
        copy(src1, prev1.at[place], send3.at[k], recv3.at[place], above + lax.rem(place + k, PLANE))
        for k in range(PLANE)]
    for item in plane_copies[PLANE - 1:] + plane_copies[:PLANE - 1]:
        item.start()
    dots(blocks - 1)
    tile_at = lambda k: acc_j[48 * k:48 * k + 24] + acc_j[48 * k + 24:48 * k + 48]
    near_force[0] = tile_at(1)
    near_force[1] = tile_at(2)
    far_force[...] = tile_at(3)
    near_copy = copy(near_force, near_in, force_send.at[0], force_recv.at[0], at(1))
    far_copy = copy(far_force, far_in, force_send.at[1], force_recv.at[1], at(2))
    far_copy.start()
    near_copy.start()
    tiles = [tile_at(0), near_force[0]]
    pad = jnp.zeros((24, L - half_c), F32)
    mi = [acc_i[48 * k:48 * k + 24] + acc_i[48 * k + 24:48 * k + 48] for k in range(2)]
    mi = [jnp.concatenate([v, pad], axis=1) for v in mi]
    hal1 = jnp.concatenate([halo_ref[...], jnp.full((1, L - fars), 4 * L, I32)], axis=1)
    oh_far = (jnp.broadcast_to(hal1, (clusters, L)) == iota((clusters, L), 0)).astype(F32).astype(BF16)

    hear(rounds - 1)
    for k in range(1, PLANE):
        other = lax.rem(place + k, PLANE)
        copy(src1, sum1.at[other], send1.at[k - 1], recv1.at[other], mates[k - 1]).wait_recv()
    row = sum1[0]
    for k in range(1, PLANE):
        row = row + sum1[k]
    src2[...] = row
    sum2[plane] = src2[...]
    column_copies = [
        copy(src2, sum2.at[plane], send2.at[k], recv2.at[plane], other) for k, other in enumerate(columns)]
    for item in column_copies:
        item.start()

    below = lax.rem(plane + planes - 1, planes)
    near_copy.wait()
    far_copy.wait()
    ff = far_in[...]
    f1 = ff.astype(BF16)
    r1 = ff - f1.astype(F32)
    f2 = r1.astype(BF16)
    f3 = (r1 - f2.astype(F32)).astype(BF16)
    far = sum(lax.dot_general(f, oh_far, (((1,), (1,)), ((), ())), preferred_element_type=F32) for f in (f3, f2, f1))
    tiles[0] = tiles[0] + far[:, 0:L]
    tiles[1] = tiles[1] + jnp.concatenate([far[:, L:], jnp.zeros((24, 2 * L - clusters), F32)], axis=1)
    back = [near_in[0], near_in[1]]
    pick = sub == (lane8 & 7)
    for c in range(3):
        for t in range(tiles_of):
            def window(tabs, slot, size):
                return take(tabs[slot // size][8 * c:8 * c + 8], slot % size + lane8 // 8)
            got = window(tiles, 16 * t, L) - window(mi, 16 * t, half_c) + window(back, half + 16 * t, L)
            force_ref[c:c + 1, t * L:(t + 1) * L] = jnp.sum(jnp.where(pick, got, 0.0), axis=0, keepdims=True)

    for item in plane_copies:
        item.wait_send()
    for k in range(PLANE):
        other = lax.rem(place + k, PLANE)
        copy(src1, prev1.at[other], send3.at[k], recv3.at[other], below * PLANE + other).wait_recv()
    row = prev1[0]
    for k in range(1, PLANE):
        row = row + prev1[k]
    sum2[below] = row
    for k, step_ in enumerate(steps):
        other = lax.rem(plane + planes - step_, planes)
        copy(src2, sum2.at[other], send2.at[k], recv2.at[other], columns[k]).wait_recv()
    row = sum2[0]
    for k in range(1, planes):
        row = row + sum2[k]
    row = jnp.broadcast_to(row, (8, L))
    one_of = [take(row, jnp.full((8, L), c, I32)) for c in range(6)]
    total = one_of[0] + one_of[1] + one_of[2]
    volume = box[0] * box[1] * box[2]
    ratio = 2.0 * total / (3.0 * (8 * clusters * domains) * thermal_scale_unit)
    coef = ext_ref[0] + reservoir_inertia_mass * (ratio - 1.0)
    for c in range(3):
        rate = ext_ref[1 + c] + barostat_gain * (
            one_of[c] - one_of[3 + c] - pressure_target * volume / 2.0
        ) / (total / 3.0)
        coef = jnp.where(sub == 1 + c, rate, coef)
    coef_ref[...] = coef
    for item in column_copies:
        item.wait_send()


def update_kernel(force_in, coef_ref, pos_ref, vel_ref, par_ref, force_ref, nvel_ref, npos_ref, coup_ref):
    coef = coef_ref[...]
    for k in range(4):
        coup_ref[k] = coef[k, 0]
    drag, grow = coef[0:1] + coef[1:4], 1.0 + time_step * coef[1:4]
    for t in range(pos_ref.shape[1] // L):
        cols = slice(t * L, (t + 1) * L)
        f, v = force_in[:, cols], vel_ref[:, cols]
        v = v + time_step * (f * par_ref[3:4, cols] - drag * v)
        force_ref[:, cols] = f
        nvel_ref[:, cols] = v
        npos_ref[:, cols] = pos_ref[:, cols] * grow + time_step * v


def on_device(
    positions,
    velocities,
    atom_params,
    pair_list,
    pair_count,
    exclusion,
    halo_far,
    box_lengths,
    extended_variables,
):
    domains = lax.axis_size("gx")
    planes = domains // PLANE
    atoms, fars = positions.shape[1], halo_far.shape[0]
    clusters, groups = atoms // 8, WIDTH // L
    vmem = pl.BlockSpec(memory_space=pltpu.VMEM)
    rows = jax.ShapeDtypeStruct((3, atoms), F32)
    dma = pltpu.SemaphoreType.DMA
    forces, coef = pl.pallas_call(
        functools.partial(step_kernel, domains),
        out_shape=(rows, jax.ShapeDtypeStruct((8, L), F32)),
        in_specs=[pl.BlockSpec(memory_space=pltpu.HBM)] * 9,
        out_specs=(vmem, vmem),
        scratch_shapes=[
            pltpu.SMEM((1,), I32),
            pltpu.SMEM((3,), F32),
            pltpu.SMEM((4,), F32),
            pltpu.VMEM((1, fars), I32),
            pltpu.VMEM((3, atoms), F32),
            pltpu.VMEM((3, atoms), F32),
            pltpu.VMEM((4, atoms), F32),
            pltpu.VMEM(pair_list.shape, I32),
            pltpu.VMEM(exclusion.shape, I32),
            pltpu.VMEM((6, 8, L), F32),
            pltpu.VMEM((3, 8, L), F32),
            pltpu.VMEM((6, 8, L), F32),
            pltpu.VMEM((3, 8, L), F32),
            pltpu.VMEM((2, 24, L), F32),
            pltpu.VMEM((24, L), F32),
            pltpu.VMEM((2, 24, L), F32),
            pltpu.VMEM((24, L), F32),
            pltpu.VMEM((8, L), F32),
            pltpu.VMEM((1, L), F32),
            pltpu.VMEM((1, L), F32),
            pltpu.VMEM((PLANE, 1, L), F32),
            pltpu.VMEM((PLANE, 1, L), F32),
            pltpu.VMEM((planes, 1, L), F32),
            pltpu.VMEM((6, 8, 2 * L), F32),
            pltpu.VMEM((4, 6, 8, L), F32),
            pltpu.VMEM((groups, 6, 16, L), F32),
            pltpu.VMEM((groups, 6, 8, L), F32),
            pltpu.VMEM((groups, 8, L), I32),
            pltpu.VMEM((groups, 6, 8, L), F32),
            pltpu.VMEM((192, L), F32),
            pltpu.VMEM((96, clusters // 2), F32),
            pltpu.VMEM((3, 8, L), F32),
            dma((9,)),
            dma((3,)),
            dma((3,)),
            dma((2,)),
            dma((2,)),
            dma((PLANE - 1,)),
            dma((PLANE,)),
            dma((PLANE,)),
            dma((PLANE,)),
            dma((planes - 2,)),
            dma((planes,)),
            pltpu.SemaphoreType.REGULAR((2 * planes.bit_length(),)),
        ],
        compiler_params=pltpu.CompilerParams(
            collective_id=0, has_side_effects=True, vmem_limit_bytes=50000 * 1024),
        name="force_step",
    )(pair_count, *[pltpu.with_memory_space_constraint(x, pltpu.HBM) for x in (box_lengths, extended_variables, halo_far[None], positions, velocities, atom_params,
      pair_list, exclusion)])
    return pl.pallas_call(
        update_kernel,
        out_shape=(rows, rows, rows, jax.ShapeDtypeStruct((4,), F32)),
        in_specs=[vmem] * 5,
        out_specs=(vmem, vmem, vmem, pl.BlockSpec(memory_space=pltpu.SMEM)),
        compiler_params=pltpu.CompilerParams(vmem_limit_bytes=8000 * 1024),
        name="update",
    )(forces, coef, positions, velocities, atom_params)


def solution(mesh):
    whole = ("rep", "gx")
    rows, flat = P(None, whole), P(whole)
    return jax.shard_map(
        on_device,
        mesh=mesh,
        in_specs=(rows, rows, rows, rows, flat, rows, flat, P("rep"), P("rep")),
        out_specs=(rows, rows, rows, P("rep")),
        check_vma=False,
    )
```
